32 devices in a mesh: dp: 4 (over y, x), group: 8 (over z, core).
Axes of the slice: x: 2, y: 2, z: 4, core: 2. Of those that a mesh axis runs over, the one named last changes fastest.
Arguments:
- tokens: bfloat16 [2048, 5120], P('dp'), may hold values from -6 to 6
- frame_mask: int32 [2048], P('dp'), may hold values 0 or 1
- cotangent: bfloat16 [2048, 5120], P('dp'), may hold values from -0.625 to 0.625
- up_weight: bfloat16 [5120, 8192], P('dp', 'group'), may hold values from -0.078125 to 0.078125
- down_weight: bfloat16 [5120, 8192], P('dp', 'group'), may hold values from -0.0625 to 0.0625
- snap_params: bfloat16 [8, 32768], P(None, ('dp', 'group')), may hold values from -6 to 6
- first_moment: float32 [8, 32768], P(None, ('dp', 'group')), may hold values from -6 to 6
- second_moment: float32 [8, 32768], P(None, ('dp', 'group')), may hold values from 0.01 to 4
- range_of_writer: int32 [8], replicated, may hold values from 0 to 7, each once
Outputs:
- grad_up: float32 [5120, 8192], P('dp', 'group')
- grad_down: float32 [5120, 8192], P('dp', 'group')
- written_params: bfloat16 [8, 32768], P('group', 'dp')
- written_moments: float32 [2, 8, 32768], P(None, 'group', 'dp')
The draws below stay inside these ranges and needn't reach their ends.
Inputs may be any that keep to these rules, and one draw needn't show every extreme that they name: `range_of_writer`: each of the 8 ranges is named by exactly one owner.
All inputs are finite; a program needn't handle non-finite values. No bound on the sum of `frame_mask` on one device may be relied on, other than what follows from the above.
Results may differ from the reference program's by a relative error of at most 0.017.
Values may be sent and summed in bfloat16 or wider, within the bound.
A program may use at most 128 MiB of HBM per device.

```python
import math
import jax
import jax.numpy as jnp
from jax import lax

D = 5120
FF = 8192
TOK_DEV = 512
TOKENS = 2048
RANGES = 8
FLAT = 32768
N_DP = 4
N_GROUP = 8


def set_ends(values, own_key, low, top_value):
    spot = [jax.random.randint(jax.random.fold_in(own_key, axis), (), 0, length) for axis, length in enumerate(values.shape)]
    widest = values.shape.index(max(values.shape))
    beside = spot[:widest] + [(spot[widest] + 1) % values.shape[widest]] + spot[widest + 1:]
    return values.at[tuple(spot)].set(low).at[tuple(beside)].set(top_value)


def raised(entries, key, source, target, blocks, factor):
    owner, partner = [(jnp.arange(entries.shape[axis_at]) // (entries.shape[axis_at] // blocks)).reshape([-1 if axis == axis_at else 1 for axis in range(entries.ndim)]) for axis_at in (source, target)]
    chosen = jax.random.permutation(key, blocks)[partner]
    strong = (owner == chosen) | (owner == (partner + blocks // 2) % blocks)
    return jnp.where(strong, factor * entries, entries)


def levels(rng, shape, cuts, smallest, largest):
    loudness = 1.0
    for dim, shards_of in cuts:
        heights = jax.random.uniform(jax.random.fold_in(jax.random.fold_in(rng, 6), dim), (shards_of,), jnp.float32, smallest / len(cuts), largest / len(cuts))
        loudness = loudness * jnp.repeat(jnp.exp(heights), shape[dim] // shards_of).reshape((-1,) + (1,) * (len(shape) - 1 - dim))
    return loudness


def bell_draw(key, dims, deviation, most, cuts=(), held_as=jnp.bfloat16):
    level = levels(key, dims, cuts, -0.22, 0.18) if cuts else 1.0
    drawn = jax.random.normal(key, dims, jnp.float32) * deviation * level
    return jnp.minimum(jnp.maximum(drawn, -most), most).astype(held_as)


def bell_draw_with(own_key, shape, deviation, reach, split, heavy, kind=jnp.bfloat16):
    array = deviation * jax.random.normal(own_key, shape, jnp.float32)
    if split:
        array = array * levels(own_key, shape, split, -0.22, 0.18)
    return jnp.clip(raised(array, jax.random.fold_in(own_key, 3), *heavy), -reach, reach).astype(kind)


def setup_inputs(seed: int = 0) -> dict:
    seeds = jax.random.split(jax.random.key(seed), 10)
    return {
        "tokens": bell_draw(seeds[0], (TOKENS, D), 1.0, 6.0, ((0, 4),)),
        "frame_mask": set_ends((jax.random.randint(seeds[1], (TOKENS,), 0, 4) < 3).astype(jnp.int32), jax.random.fold_in(seeds[1], 1), 0, 1),
        "cotangent": bell_draw_with(seeds[2], (TOKENS, D), 0.03, 0.625, ((0, 4),), (0, 1, 4, 2.0)),
        "up_weight": bell_draw(seeds[3], (D, FF), D ** -0.5, 0.078125, ((0, 4), (1, 8))),
        "down_weight": bell_draw(seeds[4], (D, FF), FF ** -0.5, 0.0625, ((0, 4), (1, 8))),
        "snap_params": bell_draw(seeds[5], (RANGES, FLAT), 0.5, 6.0, ((1, 32),)),
        "first_moment": bell_draw(seeds[6], (RANGES, FLAT), 0.5, 6.0, ((1, 32),), jnp.float32),
        "second_moment": jnp.clip(jnp.exp(math.log(4.0) - 5.9914646 * jax.random.uniform(seeds[7], (RANGES, FLAT), jnp.float32) ** levels(seeds[7], (RANGES, FLAT), ((1, 32),), -0.2, 0.2)), 0.01, 4.0),
        "range_of_writer": jax.random.permutation(seeds[8], N_GROUP).astype(jnp.int32),
    }


EPS = 1e-06

def normalize(tokens):
    values = tokens.astype(jnp.float32)
    centred = values - lax.optimization_barrier(jnp.mean(values, axis=1, keepdims=True))
    spread = lax.optimization_barrier(jnp.mean(centred * centred, axis=1, keepdims=True))
    return (centred * lax.rsqrt(spread + EPS)).astype(jnp.bfloat16)

def gelu_pair(pre, d_act):
    act, pullback = jax.vjp(lambda v: jax.nn.gelu(v, approximate=True), pre)
    return (act.astype(jnp.bfloat16), pullback(d_act)[0].astype(jnp.bfloat16))

def outer_sum(left, right):
    return lax.dot_general(left, right, (((0,), (0,)), ((), ())), preferred_element_type=jnp.float32)

def reference(tokens, frame_mask, cotangent, up_weight, down_weight, snap_params, first_moment, second_moment, range_of_writer):
    normed = normalize(tokens)
    masked = cotangent * frame_mask[:, None].astype(jnp.bfloat16)
    pre = jnp.dot(normed, up_weight, preferred_element_type=jnp.float32)
    d_act = jnp.dot(masked, down_weight, preferred_element_type=jnp.float32)
    act, grad_pre = gelu_pair(pre, d_act)
    blocks = (normed.reshape(N_DP, TOK_DEV, D), grad_pre.reshape(N_DP, TOK_DEV, FF), masked.reshape(N_DP, TOK_DEV, D), act.reshape(N_DP, TOK_DEV, FF))

    def accumulate(totals, block):
        n_blk, g_blk, m_blk, a_blk = block
        up_part = lax.optimization_barrier(outer_sum(n_blk, g_blk).astype(jnp.bfloat16)).astype(jnp.float32)
        down_part = lax.optimization_barrier(outer_sum(m_blk, a_blk).astype(jnp.bfloat16)).astype(jnp.float32)
        return ((totals[0] + up_part, totals[1] + down_part), None)
    empty = jnp.zeros((D, FF), jnp.float32)
    (grad_up, grad_down), _ = lax.scan(accumulate, (empty, empty), blocks)
    order = range_of_writer.astype(jnp.int32)
    written_params = snap_params[order]
    written_moments = jnp.stack([first_moment[order], second_moment[order]])
    return (grad_up, grad_down, written_params, written_moments)
```

```python
import functools

import jax
import jax.numpy as jnp
from jax import lax
from jax.experimental import pallas as pl
from jax.experimental.pallas import tpu as pltpu
from jax.sharding import PartitionSpec as P

EPS = 1e-06
VMEM_LIMIT = 67_000_000


def normalize(tokens):
    values = tokens.astype(jnp.float32)
    centred = values - jnp.mean(values, axis=1, keepdims=True)
    spread = jnp.mean(centred * centred, axis=1, keepdims=True)
    return (centred * lax.rsqrt(spread + EPS)).astype(jnp.bfloat16)


def gelu_pair(pre, d_act):
    act, pullback = jax.vjp(lambda v: jax.nn.gelu(v, approximate=True), pre)
    return (act.astype(jnp.bfloat16), pullback(d_act)[0].astype(jnp.bfloat16))


def outer_sum(left, right):
    return lax.dot_general(
        left, right, (((0,), (0,)), ((), ())), preferred_element_type=jnp.float32
    )


def regroup(snap_params, first_moment, second_moment, range_of_writer):
    flat = snap_params.shape[1]
    held = jnp.concatenate(
        [snap_params, first_moment.astype(jnp.bfloat16), second_moment.astype(jnp.bfloat16)],
        axis=1,
    )
    send = jnp.take(held, range_of_writer, axis=0).reshape(-1, 3, flat)
    got = lax.all_to_all(send, "group", split_axis=0, concat_axis=0, tiled=True)
    lines = jnp.swapaxes(got, 0, 1).reshape(3, 1, -1)
    return lines[0], lines[1:].astype(first_moment.dtype)


def matmul(left, right):
    return jnp.dot(left, right, preferred_element_type=jnp.float32)


def own_part(values, parts, part):
    rows = values.shape[0] // parts
    return lax.dynamic_slice_in_dim(values, part * rows, rows, axis=0)


def rounded_sum(left, right):
    total = left.astype(jnp.float32) + right.astype(jnp.float32)
    return total.astype(jnp.bfloat16)


def fits_square(tokens, up_weight):
    shares = lax.axis_size("group")
    rows, features = tokens.shape
    return (
        lax.axis_size("dp") == 4
        and shares in (2, 4, 8)
        and rows % (32 * shares) == 0
        and up_weight.shape[0] * 4 == features
        and up_weight.shape[0] % 256 == 0
        and up_weight.shape[1] % 256 == 0
    )


def flipped(index, mask, size):
    out, bit = index, 1
    while bit < size:
        out = out + bit * ((mask // bit) % 2) * (1 - 2 * ((index // bit) % 2))
        bit *= 2
    return out


def gelu_parts(pre, d_act):
    scale, cubic = 0.7978845608028654, 0.044715
    square = pre * pre
    wave = jnp.tanh(scale * (pre + cubic * (square * pre)))
    half = 0.5 * (1.0 + wave)
    slope = half + 0.5 * pre * (1.0 - wave * wave) * (scale * (1.0 + 3.0 * cubic * square))
    return pre * half, d_act * slope


def scratch(shares, rows, cols, units, flat):
    half, bf16, f32 = rows // 2, jnp.bfloat16, jnp.float32
    dma = pltpu.SemaphoreType.DMA
    return {
        "feats": pltpu.VMEM((2, shares, 4, rows, cols), bf16),
        "weights": pltpu.VMEM((2, cols, units), bf16),
        "lines": pltpu.VMEM((2, rows, 4 * cols), bf16),
        "piece": pltpu.VMEM((rows, 4 * cols), bf16),
        "own": pltpu.VMEM((shares * rows, cols), bf16),
        "staged": pltpu.VMEM((2, 4, rows, cols), bf16),
        "far_x": pltpu.VMEM((shares, 2, 2, half, units), bf16),
        "far_y": pltpu.VMEM((shares, 2, 2, half, units), bf16),
        "kept": pltpu.VMEM((shares, 2, rows, units), bf16),
        "mid_x": pltpu.VMEM((shares, 2, half, units), bf16),
        "mid_y": pltpu.VMEM((shares, 2, half, units), bf16),
        "got_x": pltpu.VMEM((shares, 2, 2, half, units), bf16),
        "got_y": pltpu.VMEM((shares, 2, 2, half, units), bf16),
        "last_x": pltpu.VMEM((shares, 2, half, units), bf16),
        "last_y": pltpu.VMEM((shares, 2, half, units), bf16),
        "wide": pltpu.VMEM((shares, 2, 4, rows, units), bf16),
        "total": pltpu.VMEM((2, cols, units), f32),
        "snap_out": pltpu.VMEM((shares, 3, 1, flat), f32),
        "snap_in": pltpu.VMEM((shares, 3, 1, flat), f32),
        "load_sem": dma((2,)),
        "weight_sem": dma((2,)),
        "block_sem": dma((2,)),
        "cross_send": dma((2, 4)),
        "cross_got": dma((2, 4)),
        "line_send": dma((2, shares)),
        "twin_send": dma((2, shares)),
        "feat_got": dma((2, shares)),
        "far_send": dma((2, 2, shares)),
        "far_got": dma((2, 2, shares)),
        "last_send": dma((2, shares)),
        "last_got": dma((2, shares)),
        "wide_send": dma((2, shares)),
        "wide_got": dma((2, shares)),
        "over_send": dma((2, shares)),
        "over_got": dma((2, shares)),
        "snap_send": dma((shares,)),
        "snap_got": dma((shares,)),
        "out_sem": dma((2, cols // 256)),
    }


def step_kernel(names, shares, *refs):
    tokens, cotangent, up_weight, down_weight, mask, snap_params, first_moment, second_moment = refs[:8]
    writer, grad_up, grad_down, out_params, out_moments = refs[8:13]
    s = dict(zip(names, refs[13:]))
    feats, weights, wide, total = s["feats"], s["weights"], s["wide"], s["total"]
    me, group = lax.axis_index("dp"), lax.axis_index("group")
    square = [me, me + 1 - 2 * (me % 2), me + 2 - 4 * (me // 2), 3 - me]
    twin = flipped(group, 1, shares)
    rows, cols, units = feats.shape[3], feats.shape[4], weights.shape[2]
    half, tile = rows // 2, 256
    bf16, f32 = jnp.bfloat16, jnp.float32
    top, low = pl.ds(0, half), pl.ds(half, half)

    def send(src, dst, send_sem, got_sem, dp_to, group_to):
        return pltpu.make_async_remote_copy(
            src_ref=src,
            dst_ref=dst,
            send_sem=send_sem,
            recv_sem=got_sem,
            device_id=(dp_to, group_to),
            device_id_type=pl.DeviceIdType.MESH,
        )

    barrier = pltpu.get_barrier_semaphore()
    partners = [(d, group) for d in square[1:]]
    partners += [(me, flipped(group, k, shares)) for k in range(1, shares)]
    for there in partners:
        pl.semaphore_signal(
            barrier, inc=1, device_id=there, device_id_type=pl.DeviceIdType.MESH
        )

    def piece_at(k):
        return pl.ds(pl.multiple_of(flipped(group, k, shares) * rows, rows), rows)

    def load_lines(k):
        return pltpu.make_async_copy(
            tokens.at[piece_at(k)], s["lines"].at[k % 2], s["load_sem"].at[k % 2]
        )

    own_columns = pl.ds(pl.multiple_of(me * cols, cols), cols)
    load_piece = pltpu.make_async_copy(
        cotangent.at[piece_at(0)], s["piece"], s["block_sem"].at[0]
    )
    load_own = pltpu.make_async_copy(cotangent.at[:, own_columns], s["own"], s["block_sem"].at[1])
    load_weights = [
        pltpu.make_async_copy(w, weights.at[t], s["weight_sem"].at[t])
        for t, w in enumerate((up_weight, down_weight))
    ]
    load_lines(0).start()
    load_piece.start()
    for copy in load_weights:
        copy.start()
    load_own.start()

    def normal_rows(k, store):
        step = 16

        def some(i, carry):
            here = pl.ds(pl.multiple_of(i * step, step), step)
            values = s["lines"][k % 2, here].astype(f32)
            centred = values - jnp.mean(values, axis=1, keepdims=True)
            spread = jnp.mean(centred * centred, axis=1, keepdims=True)
            store(here, centred, lax.rsqrt(spread + EPS))
            return carry

        lax.fori_loop(0, rows // step, some, 0)

    def cross(t, r):
        return send(
            s["staged"].at[t, square[r]],
            feats.at[t, 0, r],
            s["cross_send"].at[t, r],
            s["cross_got"].at[t, r],
            square[r],
            group,
        )

    def store_staged(here, centred, scale):
        for j in range(4):
            block = centred[:, j * cols : (j + 1) * cols] * scale
            s["staged"][0, j, here] = block.astype(bf16)

    load_lines(0).wait()
    normal_rows(0, store_staged)
    load_piece.wait()
    own_mask = mask[piece_at(0)].astype(bf16)
    for j in range(4):
        s["staged"][1, j] = s["piece"][:, j * cols : (j + 1) * cols] * own_mask
    pl.semaphore_wait(barrier, len(partners))
    for t in range(2):
        for r in (3, 1, 2):
            cross(t, r).start()
    load_lines(1).start()

    held = [snap_params[...].astype(f32), first_moment[...], second_moment[...]]
    for j in range(3):
        picked = jnp.zeros_like(held[j])
        for source in range(shares):
            chosen = writer[...] == source
            picked = jnp.where(chosen, held[j][source : source + 1], picked)
        for w in range(shares):
            s["snap_out"][w, j] = picked[w : w + 1]

    def regrouped(k):
        return send(
            s["snap_out"].at[flipped(group, k, shares)],
            s["snap_in"].at[group],
            s["snap_send"].at[k],
            s["snap_got"].at[k],
            me,
            flipped(group, k, shares),
        )

    for k in range(1, shares):
        regrouped(k).start()
    s["snap_in"][group] = s["snap_out"][group]

    def along(t, k):
        return send(
            feats.at[t, 0, pl.ds(1, 3)],
            feats.at[t, k, pl.ds(1, 3)],
            s["line_send"].at[t, k],
            s["feat_got"].at[t, k],
            me,
            flipped(group, k, shares),
        )

    def to_twin(t, k):
        return send(
            feats.at[t, k, pl.ds(1, 3)],
            feats.at[t, k + 1, pl.ds(1, 3)],
            s["twin_send"].at[t, k],
            s["feat_got"].at[t, k + 1],
            me,
            twin,
        )

    def start_total(m, carry):
        here = pl.ds(pl.multiple_of(m * tile, tile), tile)
        for t in range(2):
            total[t, here] = jnp.zeros((tile, units), f32)
        return carry

    lax.fori_loop(0, cols // tile, start_total, 0)
    load_own.wait()
    for t in range(2):
        feats[t, 0, 0] = s["staged"][t, me]
        for r in (3, 1, 2):
            cross(t, r).wait_recv()
        to_twin(t, 0).start()
        for k in range(2, shares, 2):
            along(t, k).start()
        load_weights[t].wait()

    def far(t, axis, k):
        pair = (s["far_x"], s["got_x"]) if axis == 0 else (s["far_y"], s["got_y"])
        return send(
            pair[0].at[k, t],
            pair[1].at[k, t],
            s["far_send"].at[axis, t, k],
            s["far_got"].at[axis, t, k],
            square[1 + axis],
            group,
        )

    def last(axis, k):
        pair = (s["mid_y"], s["last_x"]) if axis == 0 else (s["mid_x"], s["last_y"])
        return send(
            pair[0].at[k],
            pair[1].at[k],
            s["last_send"].at[axis, k],
            s["last_got"].at[axis, k],
            square[1 + axis],
            group,
        )

    def spread(axis, k):
        return send(
            wide.at[k, :, 0],
            wide.at[k, :, 1 + axis],
            s["wide_send"].at[axis, k],
            s["wide_got"].at[axis, k],
            square[1 + axis],
            group,
        )

    def over(axis, k):
        here = low if axis == 0 else top
        return send(
            wide.at[k, :, 2 - axis, here],
            wide.at[k, :, 3, here],
            s["over_send"].at[axis, k],
            s["over_got"].at[axis, k],
            square[1 + axis],
            group,
        )

    def products(t, k):
        def column(i, carry):
            here = pl.ds(pl.multiple_of(i * tile, tile), tile)
            left = feats[t, k].reshape(4 * rows, cols)
            out = matmul(left, weights[t, :, here]).astype(bf16)
            part = [out[r * rows : (r + 1) * rows] for r in range(4)]
            s["kept"][k, t, :, here] = part[0]
            s["far_x"][k, t, 0, :, here] = part[3][:half]
            s["far_x"][k, t, 1, :, here] = part[1][:half]
            s["far_y"][k, t, 0, :, here] = part[3][half:]
            s["far_y"][k, t, 1, :, here] = part[2][half:]
            s["mid_x"][k, t, :, here] = part[2][:half]
            s["mid_y"][k, t, :, here] = part[1][half:]
            return carry

        lax.fori_loop(0, units // tile, column, 0)
        far(t, 0, k).start()
        far(t, 1, k).start()


    def own_rows(k):
        load_lines(k).wait()

        @pl.when(k + 1 < shares)
        def _():
            load_lines(k + 1).start()

        step = 16

        def some(i, carry):
            here = pl.ds(pl.multiple_of(i * step, step), step)
            values = s["lines"][k % 2, here].astype(f32)
            mean = jnp.mean(values, axis=1, keepdims=True)
            centred = values - mean
            spread_of = jnp.mean(centred * centred, axis=1, keepdims=True)
            mine = s["lines"][k % 2, here, own_columns].astype(f32) - mean
            feats[0, k, 0, here] = (mine * lax.rsqrt(spread_of + EPS)).astype(bf16)
            return carry

        lax.fori_loop(0, rows // step, some, 0)
        here = piece_at(k)
        feats[1, k, 0] = s["own"][here] * mask[here].astype(bf16)

    def stage_products(k):
        @pl.when(k > 0)
        def _():
            own_rows(k)

        for t in range(2):

            @pl.when(k > 0)
            def _():
                along(t, k).wait_recv()

            @pl.when((k > 0) & (k % 2 == 0))
            def _():
                to_twin(t, k).start()

            products(t, k)

    def stage_middle(k):
        for t in range(2):
            far(t, 0, k).wait_recv()
            s["mid_x"][k, t] = rounded_sum(s["mid_x"][k, t], s["got_x"][k, t, 0])
        last(1, k).start()
        for t in range(2):
            far(t, 1, k).wait_recv()
            s["mid_y"][k, t] = rounded_sum(s["mid_y"][k, t], s["got_y"][k, t, 0])
        last(0, k).start()

    def stage_gelu(k):
        last(1, k).wait_recv()
        last(0, k).wait_recv()
        step = 16
        for axis, near_ref, last_ref in (
            (0, s["got_x"], s["last_y"]),
            (1, s["got_y"], s["last_x"]),
        ):

            def some(i, carry):
                here = pl.ds(pl.multiple_of(i * step, step), step)
                out = pl.ds(pl.multiple_of(axis * half + i * step, step), step)
                sums = [
                    s["kept"][k, t, out].astype(f32)
                    + near_ref[k, t, 1, here].astype(f32)
                    + last_ref[k, t, here].astype(f32)
                    for t in range(2)
                ]
                act, grad_pre = gelu_parts(*sums)
                wide[k, 0, 0, out] = grad_pre.astype(bf16)
                wide[k, 1, 0, out] = act.astype(bf16)
                return carry

            lax.fori_loop(0, half // step, some, 0)
        spread(0, k).start()
        spread(1, k).start()

    def stage_over(k):
        spread(0, k).wait_recv()
        over(1, k).start()
        spread(1, k).wait_recv()
        over(0, k).start()

    def result(t, m):
        here = pl.ds(pl.multiple_of(m * tile, tile), tile)
        return pltpu.make_async_copy(
            total.at[t, here], (grad_up, grad_down)[t].at[here], s["out_sem"].at[t, m]
        )

    def stage_gradient(k):
        over(0, k).wait_recv()
        over(1, k).wait_recv()
        for t in range(2):

            def some(m, carry):
                here = pl.ds(pl.multiple_of(m * tile, tile), tile)
                left = feats[t, k, :, :, here].reshape(4 * rows, tile)
                right = wide[k, t].reshape(4 * rows, units)
                total[t, here] = total[t, here] + outer_sum(left, right)

                @pl.when(k == shares - 1)
                def _():
                    result(t, m).start()

                return carry

            lax.fori_loop(0, cols // tile, some, 0)

    stages = (stage_products, stage_middle, stage_gelu, stage_over, stage_gradient)

    def pipeline(step, carry):
        for lag, stage in enumerate(stages):

            @pl.when((step >= lag) & (step - lag < shares))
            def _():
                stage(step - lag)

        return carry

    lax.fori_loop(0, shares + len(stages) - 1, pipeline, 0)

    for k in range(1, shares):
        regrouped(k).wait()
    for source in range(shares):
        here = pl.ds(source * out_params.shape[1] // shares, out_params.shape[1] // shares)
        out_params[:, here] = s["snap_in"][source, 0].astype(out_params.dtype)
        for j in range(2):
            out_moments[j, :, here] = s["snap_in"][source, 1 + j]

    for t in range(2):
        for r in (1, 2, 3):
            cross(t, r).wait_send()
        for k in range(0, shares, 2):
            to_twin(t, k).wait_send()
        for k in range(2, shares, 2):
            along(t, k).wait_send()

    def finish(k, carry):
        for axis in range(2):
            for t in range(2):
                far(t, axis, k).wait_send()
            last(axis, k).wait_send()
            spread(axis, k).wait_send()
            over(axis, k).wait_send()
        return carry

    lax.fori_loop(0, shares, finish, 0)

    def written(m, carry):
        for t in range(2):
            result(t, m).wait()
        return carry

    lax.fori_loop(0, cols // tile, written, 0)


def weight_gradients(
    tokens,
    frame_mask,
    cotangent,
    up_weight,
    down_weight,
    snap_params,
    first_moment,
    second_moment,
    range_of_writer,
):
    shares = lax.axis_size("group")
    rows, (cols, units), flat = tokens.shape[0] // shares, up_weight.shape, snap_params.shape[1]
    buffers = scratch(shares, rows, cols, units, flat)
    anywhere = pl.BlockSpec(memory_space=pl.ANY)
    inside = pl.BlockSpec(memory_space=pltpu.VMEM)
    f32 = jnp.float32
    tall = 4 * shares * rows
    return pl.pallas_call(
        functools.partial(step_kernel, tuple(buffers), shares),
        out_shape=(
            jax.ShapeDtypeStruct((cols, units), f32),
            jax.ShapeDtypeStruct((cols, units), f32),
            jax.ShapeDtypeStruct((1, shares * flat), snap_params.dtype),
            jax.ShapeDtypeStruct((2, 1, shares * flat), first_moment.dtype),
        ),
        in_specs=[anywhere] * 4 + [inside] * 5,
        out_specs=(anywhere, anywhere, inside, inside),
        scratch_shapes=list(buffers.values()),
        compiler_params=pltpu.CompilerParams(
            collective_id=0, has_side_effects=True, vmem_limit_bytes=VMEM_LIMIT
        ),
        cost_estimate=pl.CostEstimate(
            flops=8 * tall * cols * units,
            bytes_accessed=8 * cols * units + 8 * cols * units,
            transcendentals=tall * units // 4,
        ),
        name="backward_step",
    )(
        tokens,
        cotangent,
        up_weight,
        down_weight,
        frame_mask[:, None],
        snap_params,
        first_moment,
        second_moment,
        range_of_writer[:, None],
    )


def weight_gradients_any(tokens, frame_mask, cotangent, up_weight, down_weight, *snapshot):
    shares = lax.axis_size("group")
    group = lax.axis_index("group")
    mask = own_part(frame_mask, shares, group)[:, None].astype(jnp.bfloat16)

    def to_features(rows_here):
        part = lax.all_to_all(rows_here, "dp", split_axis=1, concat_axis=0, tiled=True)
        return lax.all_gather(part, "group", axis=0, tiled=True)

    def own_rows_total(left, weight):
        part = matmul(left, weight).astype(jnp.bfloat16)
        return lax.psum_scatter(part, "dp", scatter_dimension=0, tiled=True).astype(jnp.float32)

    normed = to_features(normalize(own_part(tokens, shares, group)))
    masked = to_features(own_part(cotangent, shares, group) * mask)
    act, grad_pre = gelu_pair(
        own_rows_total(normed, up_weight), own_rows_total(masked, down_weight)
    )
    grad_down = outer_sum(masked, lax.all_gather(act, "dp", axis=0, tiled=True))
    grad_up = outer_sum(normed, lax.all_gather(grad_pre, "dp", axis=0, tiled=True))
    return grad_up, grad_down, *regroup(*snapshot)


def per_device(
    tokens,
    frame_mask,
    cotangent,
    up_weight,
    down_weight,
    snap_params,
    first_moment,
    second_moment,
    range_of_writer,
):
    square = fits_square(tokens, up_weight)
    compute = weight_gradients if square else weight_gradients_any
    snapshot = (snap_params, first_moment, second_moment, range_of_writer)
    return compute(tokens, frame_mask, cotangent, up_weight, down_weight, *snapshot)


def solution(mesh):
    placed = (
        P("dp", None),
        P("dp"),
        P("dp", None),
        P("dp", "group"),
        P("dp", "group"),
        P(None, ("dp", "group")),
        P(None, ("dp", "group")),
        P(None, ("dp", "group")),
        P(),
    )
    return jax.shard_map(
        per_device,
        mesh=mesh,
        in_specs=placed,
        out_specs=(P("dp", "group"), P("dp", "group"), P("group", "dp"), P(None, "group", "dp")),
        check_vma=False,
    )
```

```python
import functools

import jax
import jax.numpy as jnp
from jax import lax
from jax.experimental import pallas as pl
from jax.experimental.pallas import tpu as pltpu
from jax.sharding import PartitionSpec as P

EPS = 1e-06
STEP_VMEM, LAST_VMEM = 38 * 2**20, 8 * 2**20


def normalize(tokens):
    values = tokens.astype(jnp.float32)
    centred = values - jnp.mean(values, axis=1, keepdims=True)
    spread = jnp.mean(centred * centred, axis=1, keepdims=True)
    return (centred * lax.rsqrt(spread + EPS)).astype(jnp.bfloat16)


def gelu_pair(pre, d_act):
    act, pullback = jax.vjp(lambda v: jax.nn.gelu(v, approximate=True), pre)
    return (act.astype(jnp.bfloat16), pullback(d_act)[0].astype(jnp.bfloat16))


def outer_sum(left, right):
    return lax.dot_general(
        left, right, (((0,), (0,)), ((), ())), preferred_element_type=jnp.float32
    )


def regroup(snap_params, first_moment, second_moment, range_of_writer):
    flat = snap_params.shape[1]
    held = jnp.concatenate(
        [snap_params, first_moment.astype(jnp.bfloat16), second_moment.astype(jnp.bfloat16)],
        axis=1,
    )
    send = jnp.take(held, range_of_writer, axis=0).reshape(-1, 3, flat)
    got = lax.all_to_all(send, "group", split_axis=0, concat_axis=0, tiled=True)
    lines = jnp.swapaxes(got, 0, 1).reshape(3, 1, -1)
    return lines[0], lines[1:].astype(first_moment.dtype)


def matmul(left, right):
    return jnp.dot(left, right, preferred_element_type=jnp.float32)


def own_part(values, parts, part):
    rows = values.shape[0] // parts
    return lax.dynamic_slice_in_dim(values, part * rows, rows, axis=0)


def rounded_sum(left, right):
    total = left.astype(jnp.float32) + right.astype(jnp.float32)
    return total.astype(jnp.bfloat16)


def fits_square(tokens, up_weight):
    shares = lax.axis_size("group")
    rows, features = tokens.shape
    return (
        lax.axis_size("dp") == 4
        and shares == 8
        and rows % (32 * shares) == 0
        and up_weight.shape[0] * 4 == features
        and up_weight.shape[0] % 256 == 0
        and up_weight.shape[1] % 256 == 0
    )


def flipped(index, mask, size):
    out, bit = index, 1
    while bit < size:
        out = out + bit * ((mask // bit) % 2) * (1 - 2 * ((index // bit) % 2))
        bit *= 2
    return out


def line_orders(chips):
    return [sorted(range(chips), key=lambda w: (abs(w - c), w)) for c in range(chips)]


def gelu_parts(pre, d_act):
    scale, cubic = 0.7978845608028654, 0.044715
    square = pre * pre
    wave = jnp.tanh(scale * (pre + cubic * (square * pre)))
    half = 0.5 * (1.0 + wave)
    slope = half + 0.5 * pre * (1.0 - wave * wave) * (scale * (1.0 + 3.0 * cubic * square))
    return pre * half, d_act * slope


def scratch(shares, rows, cols, units, flat):
    half, bf16, f32 = rows // 2, jnp.bfloat16, jnp.float32
    dma = pltpu.SemaphoreType.DMA
    return {
        "feats": pltpu.VMEM((2, shares, 4, rows, cols), bf16),
        "weights": pltpu.VMEM((2, cols, units), bf16),
        "lines": pltpu.VMEM((2, rows, 4 * cols), bf16),
        "piece": pltpu.VMEM((rows, 4 * cols), bf16),
        "own": pltpu.VMEM((shares * rows, cols), bf16),
        "staged": pltpu.VMEM((2, 4, rows, cols), bf16),
        "far_x": pltpu.VMEM((shares, 2, 2, half, units), bf16),
        "far_y": pltpu.VMEM((shares, 2, 2, half, units), bf16),
        "kept": pltpu.VMEM((shares, 2, rows, units), bf16),
        "mid_x": pltpu.VMEM((shares, 2, half, units), bf16),
        "mid_y": pltpu.VMEM((shares, 2, half, units), bf16),
        "got_x": pltpu.VMEM((shares, 2, 2, half, units), bf16),
        "got_y": pltpu.VMEM((shares, 2, 2, half, units), bf16),
        "last_x": pltpu.VMEM((shares, 2, half, units), bf16),
        "last_y": pltpu.VMEM((shares, 2, half, units), bf16),
        "snap_out": pltpu.VMEM((shares, 3, 1, flat), f32),
        "load_sem": dma((2,)),
        "weight_sem": dma((2,)),
        "block_sem": dma((2,)),
        "cross_send": dma((2, 4)),
        "cross_got": dma((2, 4)),
        "line_send": dma((2, 2, shares // 2)),
        "twin_send": dma((2, shares)),
        "feat_got": dma((2, shares)),
        "far_send": dma((2, 2, shares)),
        "far_got": dma((2, 2, shares)),
        "last_send": dma((2, shares)),
        "last_got": dma((2, shares)),
        "wide_send": dma((2, shares)),
        "wide_got": dma((2, shares)),
        "over_send": dma((2, shares)),
        "over_got": dma((2, shares)),
        "snap_send": dma((shares,)),
        "snap_got": dma((shares,)),
    }


def step_kernel(names, shares, *refs):
    tokens, cotangent, up_weight, down_weight, mask, snap_params, first_moment, second_moment = refs[:8]
    writer, *total, last_feats, wide, snap_in = refs[8:14]
    s = dict(zip(names, refs[14:]))
    feats, weights = s["feats"], s["weights"]
    me, group = lax.axis_index("dp"), lax.axis_index("group")
    square = [me, me + 1 - 2 * (me % 2), me + 2 - 4 * (me // 2), 3 - me]
    twin = flipped(group, 1, shares)
    chip, core = group // 2, group % 2
    orders = line_orders(shares // 2)
    inner = range(1, len(orders) - 1)
    outer = (0, len(orders) - 1)
    table = sum(w << (8 * c + 2 * p) for c, order in enumerate(orders) for p, w in enumerate(order))
    own_order = table // ((1 + 255 * (chip % 2)) * (1 + 65535 * (chip // 2))) % 256
    rows, cols, units = feats.shape[3], feats.shape[4], weights.shape[2]
    half, tile = rows // 2, 256
    bf16, f32 = jnp.bfloat16, jnp.float32
    top, low = pl.ds(0, half), pl.ds(half, half)

    def send(src, dst, send_sem, got_sem, dp_to, group_to):
        return pltpu.make_async_remote_copy(
            src_ref=src,
            dst_ref=dst,
            send_sem=send_sem,
            recv_sem=got_sem,
            device_id=(dp_to, group_to),
            device_id_type=pl.DeviceIdType.MESH,
        )

    barrier = pltpu.get_barrier_semaphore()
    partners = [(d, group) for d in square[1:]]
    partners += [(me, flipped(group, k, shares)) for k in range(1, shares)]
    for there in partners:
        pl.semaphore_signal(
            barrier, inc=1, device_id=there, device_id_type=pl.DeviceIdType.MESH
        )

    def owner_of(k):
        place = k // 2
        there = own_order // ((1 + 3 * (place % 2)) * (1 + 15 * (place // 2))) % 4
        return 2 * there + (core + k) % 2

    def piece_at(k):
        return pl.ds(pl.multiple_of(owner_of(k) * rows, rows), rows)

    def mask_column(k):
        shape = (rows, mask.shape[1])
        at = lax.broadcasted_iota(jnp.int32, shape, 0) + owner_of(k) * rows
        chosen = at == lax.broadcasted_iota(jnp.int32, shape, 1)
        entries = jnp.where(chosen, jnp.broadcast_to(mask[...].astype(f32), shape), 0.0)
        return jnp.sum(entries, axis=1, keepdims=True).astype(bf16)

    def load_lines(k):
        return pltpu.make_async_copy(
            tokens.at[piece_at(k)], s["lines"].at[k % 2], s["load_sem"].at[k % 2]
        )

    own_columns = pl.ds(pl.multiple_of(me * cols, cols), cols)
    load_piece = pltpu.make_async_copy(
        cotangent.at[piece_at(0)], s["piece"], s["block_sem"].at[0]
    )
    load_own = pltpu.make_async_copy(cotangent.at[:, own_columns], s["own"], s["block_sem"].at[1])
    load_weights = [
        pltpu.make_async_copy(w, weights.at[t], s["weight_sem"].at[t])
        for t, w in enumerate((up_weight, down_weight))
    ]
    load_piece.start()
    load_lines(0).start()
    for copy in load_weights:
        copy.start()
    load_own.start()

    def normal_rows(k, store):
        step = 16

        def some(i, carry):
            here = pl.ds(pl.multiple_of(i * step, step), step)
            values = s["lines"][k % 2, here].astype(f32)
            centred = values - jnp.mean(values, axis=1, keepdims=True)
            spread = jnp.mean(centred * centred, axis=1, keepdims=True)
            store(here, centred, lax.rsqrt(spread + EPS))
            return carry

        lax.fori_loop(0, rows // step, some, 0)

    def cross(t, r):
        return send(
            s["staged"].at[t, square[r]],
            feats.at[t, 0, r],
            s["cross_send"].at[t, r],
            s["cross_got"].at[t, r],
            square[r],
            group,
        )

    def store_staged(here, centred, scale):
        for j in range(4):
            block = centred[:, j * cols : (j + 1) * cols] * scale
            s["staged"][0, j, here] = block.astype(bf16)

    load_piece.wait()
    own_mask = mask_column(0)
    for j in range(4):
        s["staged"][1, j] = s["piece"][:, j * cols : (j + 1) * cols] * own_mask
    pl.semaphore_wait(barrier, len(partners))
    for r in (3, 1, 2):
        cross(1, r).start()
    load_lines(0).wait()
    normal_rows(0, store_staged)
    for r in (3, 1, 2):
        cross(0, r).start()
    load_lines(1).start()

    held = [snap_params[...].astype(f32), first_moment[...], second_moment[...]]
    for w in range(shares):
        for j in range(3):
            picked = jnp.zeros((1, held[j].shape[1]), f32)
            for source in range(shares):
                picked = jnp.where(writer[w] == source, held[j][source : source + 1], picked)
            s["snap_out"][w, j] = picked

    def regrouped(k):
        return send(
            s["snap_out"].at[flipped(group, k, shares)],
            snap_in.at[group],
            s["snap_send"].at[k],
            s["snap_got"].at[k],
            me,
            flipped(group, k, shares),
        )

    for k in range(1, shares):
        regrouped(k).start()
    snap_in[group] = s["snap_out"][group]

    def onward(t, c, w, way):
        place, there = orders[c].index(w), orders[c + way].index(w)
        return send(
            feats.at[t, 2 * place, pl.ds(1, 3)],
            feats.at[t, 2 * there, pl.ds(1, 3)],
            s["line_send"].at[t, (way + 1) // 2, place],
            s["feat_got"].at[t, 2 * there],
            me,
            group + 2 * way,
        )

    def moves(c, place):
        w = orders[c][place]
        ways = [way for way, goes in ((-1, w >= c), (1, w <= c)) if goes]
        return [(w, way) for way in ways if 0 <= c + way < len(orders)]

    def move_on(t, chips, place):
        for c in chips:

            @pl.when(chip == c)
            def _():
                for w, way in moves(c, place):
                    onward(t, c, w, way).start()

    def arrived(t, k):
        return to_twin(t, k - 1).wait_recv()

    def to_twin(t, k):
        return send(
            feats.at[t, k, pl.ds(1, 3)],
            feats.at[t, k + 1, pl.ds(1, 3)],
            s["twin_send"].at[t, k],
            s["feat_got"].at[t, k + 1],
            me,
            twin,
        )

    def start_total(m, carry):
        here = pl.ds(pl.multiple_of(m * tile, tile), tile)
        for t in range(2):
            total[t][here] = jnp.zeros((tile, units), f32)
        return carry

    lax.fori_loop(0, cols // tile, start_total, 0)
    load_own.wait()
    for t in (1, 0):
        feats[t, 0, 0] = s["staged"][t, me]
        for r in (3, 1, 2):
            cross(t, r).wait_recv()
        move_on(t, range(len(orders)), 0)
        to_twin(t, 0).start()
        load_weights[t].wait()

    def far(t, axis, k):
        pair = (s["far_x"], s["got_x"]) if axis == 0 else (s["far_y"], s["got_y"])
        return send(
            pair[0].at[k, t],
            pair[1].at[k, t],
            s["far_send"].at[axis, t, k],
            s["far_got"].at[axis, t, k],
            square[1 + axis],
            group,
        )

    def last(axis, k):
        pair = (s["mid_y"], s["last_x"]) if axis == 0 else (s["mid_x"], s["last_y"])
        return send(
            pair[0].at[k],
            pair[1].at[k],
            s["last_send"].at[axis, k],
            s["last_got"].at[axis, k],
            square[1 + axis],
            group,
        )

    def spread(axis, k):
        return send(
            wide.at[k, :, 0],
            wide.at[k, :, 1 + axis],
            s["wide_send"].at[axis, k],
            s["wide_got"].at[axis, k],
            square[1 + axis],
            group,
        )

    def over(axis, k):
        here = low if axis == 0 else top
        return send(
            wide.at[k, :, 2 - axis, here],
            wide.at[k, :, 3, here],
            s["over_send"].at[axis, k],
            s["over_got"].at[axis, k],
            square[1 + axis],
            group,
        )

    def products(t, k):
        def column(i, carry):
            here = pl.ds(pl.multiple_of(i * tile, tile), tile)
            left = feats[t, k].reshape(4 * rows, cols)
            out = matmul(left, weights[t, :, here]).astype(bf16)
            part = [out[r * rows : (r + 1) * rows] for r in range(4)]
            s["kept"][k, t, :, here] = part[0]
            s["far_x"][k, t, 0, :, here] = part[3][:half]
            s["far_x"][k, t, 1, :, here] = part[1][:half]
            s["far_y"][k, t, 0, :, here] = part[3][half:]
            s["far_y"][k, t, 1, :, here] = part[2][half:]
            s["mid_x"][k, t, :, here] = part[2][:half]
            s["mid_y"][k, t, :, here] = part[1][half:]
            return carry

        lax.fori_loop(0, units // tile, column, 0)
        far(t, 0, k).start()
        far(t, 1, k).start()


    def own_rows(k):
        load_lines(k).wait()

        @pl.when(k + 1 < shares)
        def _():
            load_lines(k + 1).start()

        step = 16

        def some(i, carry):
            here = pl.ds(pl.multiple_of(i * step, step), step)
            values = s["lines"][k % 2, here].astype(f32)
            mean = jnp.mean(values, axis=1, keepdims=True)
            centred = values - mean
            spread_of = jnp.mean(centred * centred, axis=1, keepdims=True)
            mine = s["lines"][k % 2, here, own_columns].astype(f32) - mean
            feats[0, k, 0, here] = (mine * lax.rsqrt(spread_of + EPS)).astype(bf16)
            return carry

        lax.fori_loop(0, rows // step, some, 0)
        feats[1, k, 0] = s["own"][piece_at(k)] * mask_column(k)

    def stage_products(k):
        @pl.when(k > 0)
        def _():
            own_rows(k)

        at_end = (chip == outer[0]) | (chip == outer[1])
        within = jnp.logical_not(at_end)
        for t in (1, 0):

            @pl.when(k % 2 == 1)
            def _():
                arrived(t, k)

            @pl.when(k == 2)
            def _():
                arrived(t, 2)
                move_on(t, inner, 1)

            @pl.when((k == 2) & within)
            def _():
                arrived(t, 4)
                move_on(t, inner, 2)

            @pl.when((k == 4) & within)
            def _():
                arrived(t, 6)
                move_on(t, inner, 3)

            @pl.when((k >= 4) & (k % 2 == 0) & at_end)
            def _():
                arrived(t, k)

            @pl.when((k > 0) & (k % 2 == 0))
            def _():
                to_twin(t, k).start()

            products(t, k)

            @pl.when(k == shares - 1)
            def _():
                for r in range(4):
                    last_feats[t, r] = feats[t, k, r]

    def stage_middle(k):
        for t in range(2):
            far(t, 0, k).wait_recv()
            s["mid_x"][k, t] = rounded_sum(s["mid_x"][k, t], s["got_x"][k, t, 0])
        last(1, k).start()
        for t in range(2):
            far(t, 1, k).wait_recv()
            s["mid_y"][k, t] = rounded_sum(s["mid_y"][k, t], s["got_y"][k, t, 0])
        last(0, k).start()

    def stage_gelu(k):
        last(1, k).wait_recv()
        last(0, k).wait_recv()
        step = 16
        for axis, near_ref, last_ref in (
            (0, s["got_x"], s["last_y"]),
            (1, s["got_y"], s["last_x"]),
        ):

            def some(i, carry):
                here = pl.ds(pl.multiple_of(i * step, step), step)
                out = pl.ds(pl.multiple_of(axis * half + i * step, step), step)
                sums = [
                    s["kept"][k, t, out].astype(f32)
                    + near_ref[k, t, 1, here].astype(f32)
                    + last_ref[k, t, here].astype(f32)
                    for t in range(2)
                ]
                act, grad_pre = gelu_parts(*sums)
                wide[k, 0, 0, out] = grad_pre.astype(bf16)
                wide[k, 1, 0, out] = act.astype(bf16)
                return carry

            lax.fori_loop(0, half // step, some, 0)
        spread(0, k).start()
        spread(1, k).start()

    def stage_over(k):
        spread(0, k).wait_recv()
        over(1, k).start()
        spread(1, k).wait_recv()
        over(0, k).start()

    def stage_gradient(k):
        over(0, k).wait_recv()
        over(1, k).wait_recv()

        @pl.when(k < shares - 1)
        def _():
            for t in range(2):

                def some(m, carry):
                    here = pl.ds(pl.multiple_of(m * tile, tile), tile)
                    left = feats[t, k, :, :, here].reshape(4 * rows, tile)
                    right = wide[k, t].reshape(4 * rows, units)
                    total[t][here] = total[t][here] + outer_sum(left, right)
                    return carry

                lax.fori_loop(0, cols // tile, some, 0)

    stages = (stage_products, stage_middle, stage_gelu, stage_over, stage_gradient)

    def pipeline(step, carry):
        for lag, stage in enumerate(stages):

            @pl.when((step >= lag) & (step - lag < shares))
            def _():
                stage(step - lag)

        return carry

    lax.fori_loop(0, shares + len(stages) - 1, pipeline, 0)

    for k in range(1, shares):
        regrouped(k).wait()
    for t in range(2):
        for r in (1, 2, 3):
            cross(t, r).wait_send()
        for k in range(0, shares, 2):
            to_twin(t, k).wait_send()
        for c in range(len(orders)):

            @pl.when(chip == c)
            def _():
                for place in range(len(orders)):
                    for w, way in moves(c, place):
                        onward(t, c, w, way).wait_send()


    def finish(k, carry):
        for axis in range(2):
            for t in range(2):
                far(t, axis, k).wait_send()
            last(axis, k).wait_send()
            spread(axis, k).wait_send()
            over(axis, k).wait_send()
        return carry

    lax.fori_loop(0, shares, finish, 0)


def last_kernel(
    total_up, total_down, feats, wide, snap, grad_up, grad_down, params, moments, ready, sem
):
    shares, rows, units = wide.shape[0], feats.shape[2], wide.shape[4]
    slots, tile = ready.shape[0], ready.shape[1]
    tiles = total_up.shape[0] // tile

    def written(n):
        t, m = n // tiles, n % tiles
        return pltpu.make_async_copy(
            ready.at[n % slots],
            (grad_up, grad_down)[t].at[pl.ds(m * tile, tile)],
            sem.at[n % slots],
        )

    for n in range(2 * tiles):
        t, here = n // tiles, pl.ds(n % tiles * tile, tile)
        if n >= slots:
            written(n - slots).wait()
        left = feats[t, :, :, here].reshape(4 * rows, tile)
        right = wide[shares - 1, t].reshape(4 * rows, units)
        ready[n % slots] = (total_up, total_down)[t][here] + outer_sum(left, right)
        written(n).start()
    width = params.shape[1] // shares
    for source in range(shares):
        here = pl.ds(source * width, width)
        params[:, here] = snap[source, 0].astype(params.dtype)
        for j in range(2):
            moments[j, :, here] = snap[source, 1 + j]
    for n in range(max(0, 2 * tiles - slots), 2 * tiles):
        written(n).wait()


def weight_gradients(
    tokens,
    frame_mask,
    cotangent,
    up_weight,
    down_weight,
    snap_params,
    first_moment,
    second_moment,
    range_of_writer,
):
    shares = lax.axis_size("group")
    rows, (cols, units), flat = tokens.shape[0] // shares, up_weight.shape, snap_params.shape[1]
    buffers = scratch(shares, rows, cols, units, flat)
    anywhere = pl.BlockSpec(memory_space=pl.ANY)
    inside = pl.BlockSpec(memory_space=pltpu.VMEM)
    scalars = pl.BlockSpec(memory_space=pltpu.SMEM)
    bf16, f32 = jnp.bfloat16, jnp.float32
    piece_flops = 8 * 4 * rows * cols * units
    sums = pl.pallas_call(
        functools.partial(step_kernel, tuple(buffers), shares),
        out_shape=(
            pltpu.VMEM((cols, units), f32),
            pltpu.VMEM((cols, units), f32),
            pltpu.VMEM((2, 4, rows, cols), bf16),
            pltpu.VMEM((shares, 2, 4, rows, units), bf16),
            pltpu.VMEM((shares, 3, 1, flat), f32),
        ),
        in_specs=[anywhere] * 4 + [inside] * 4 + [scalars],
        out_specs=(inside,) * 5,
        scratch_shapes=list(buffers.values()),
        compiler_params=pltpu.CompilerParams(
            collective_id=0, has_side_effects=True, vmem_limit_bytes=STEP_VMEM
        ),
        cost_estimate=pl.CostEstimate(
            flops=shares * piece_flops,
            bytes_accessed=4 * cols * units + 4 * tokens.size,
            transcendentals=shares * rows * units,
        ),
        name="backward_step",
    )(
        tokens,
        cotangent,
        up_weight,
        down_weight,
        frame_mask[None, :],
        snap_params,
        first_moment,
        second_moment,
        range_of_writer,
    )
    tile, slots = 256, 4
    return pl.pallas_call(
        last_kernel,
        out_shape=(
            jax.ShapeDtypeStruct((cols, units), f32),
            jax.ShapeDtypeStruct((cols, units), f32),
            jax.ShapeDtypeStruct((1, shares * flat), snap_params.dtype),
            jax.ShapeDtypeStruct((2, 1, shares * flat), first_moment.dtype),
        ),
        in_specs=[inside] * 5,
        out_specs=(anywhere, anywhere, inside, inside),
        scratch_shapes=[
            pltpu.VMEM((slots, tile, units), f32),
            pltpu.SemaphoreType.DMA((slots,)),
        ],
        compiler_params=pltpu.CompilerParams(vmem_limit_bytes=LAST_VMEM),
        cost_estimate=pl.CostEstimate(
            flops=piece_flops // 2, bytes_accessed=8 * cols * units, transcendentals=0
        ),
        name="last_piece",
    )(*sums)


def weight_gradients_any(tokens, frame_mask, cotangent, up_weight, down_weight, *snapshot):
    shares = lax.axis_size("group")
    group = lax.axis_index("group")
    mask = own_part(frame_mask, shares, group)[:, None].astype(jnp.bfloat16)

    def to_features(rows_here):
        part = lax.all_to_all(rows_here, "dp", split_axis=1, concat_axis=0, tiled=True)
        return lax.all_gather(part, "group", axis=0, tiled=True)

    def own_rows_total(left, weight):
        part = matmul(left, weight).astype(jnp.bfloat16)
        return lax.psum_scatter(part, "dp", scatter_dimension=0, tiled=True).astype(jnp.float32)

    normed = to_features(normalize(own_part(tokens, shares, group)))
    masked = to_features(own_part(cotangent, shares, group) * mask)
    act, grad_pre = gelu_pair(
        own_rows_total(normed, up_weight), own_rows_total(masked, down_weight)
    )
    grad_down = outer_sum(masked, lax.all_gather(act, "dp", axis=0, tiled=True))
    grad_up = outer_sum(normed, lax.all_gather(grad_pre, "dp", axis=0, tiled=True))
    return grad_up, grad_down, *regroup(*snapshot)


def per_device(
    tokens,
    frame_mask,
    cotangent,
    up_weight,
    down_weight,
    snap_params,
    first_moment,
    second_moment,
    range_of_writer,
):
    square = fits_square(tokens, up_weight)
    compute = weight_gradients if square else weight_gradients_any
    snapshot = (snap_params, first_moment, second_moment, range_of_writer)
    return compute(tokens, frame_mask, cotangent, up_weight, down_weight, *snapshot)


def solution(mesh):
    placed = (
        P("dp", None),
        P("dp"),
        P("dp", None),
        P("dp", "group"),
        P("dp", "group"),
        P(None, ("dp", "group")),
        P(None, ("dp", "group")),
        P(None, ("dp", "group")),
        P(),
    )
    return jax.shard_map(
        per_device,
        mesh=mesh,
        in_specs=placed,
        out_specs=(P("dp", "group"), P("dp", "group"), P("group", "dp"), P(None, "group", "dp")),
        check_vma=False,
    )
```

```python
import functools

import jax
import jax.numpy as jnp
from jax import lax
from jax.experimental import pallas as pl
from jax.experimental.pallas import tpu as pltpu
from jax.sharding import PartitionSpec as P

EPS = 1e-06
STEP_VMEM, LAST_VMEM = 41 * 2**20, 8 * 2**20


def normalize(tokens):
    values = tokens.astype(jnp.float32)
    centred = values - jnp.mean(values, axis=1, keepdims=True)
    spread = jnp.mean(centred * centred, axis=1, keepdims=True)
    return (centred * lax.rsqrt(spread + EPS)).astype(jnp.bfloat16)


def gelu_pair(pre, d_act):
    act, pullback = jax.vjp(lambda v: jax.nn.gelu(v, approximate=True), pre)
    return (act.astype(jnp.bfloat16), pullback(d_act)[0].astype(jnp.bfloat16))


def outer_sum(left, right):
    return lax.dot_general(
        left, right, (((0,), (0,)), ((), ())), preferred_element_type=jnp.float32
    )


def regroup(snap_params, first_moment, second_moment, range_of_writer):
    flat = snap_params.shape[1]
    held = jnp.concatenate(
        [snap_params, first_moment.astype(jnp.bfloat16), second_moment.astype(jnp.bfloat16)],
        axis=1,
    )
    send = jnp.take(held, range_of_writer, axis=0).reshape(-1, 3, flat)
    got = lax.all_to_all(send, "group", split_axis=0, concat_axis=0, tiled=True)
    lines = jnp.swapaxes(got, 0, 1).reshape(3, 1, -1)
    return lines[0], lines[1:].astype(first_moment.dtype)


def matmul(left, right):
    return jnp.dot(left, right, preferred_element_type=jnp.float32)


def own_part(values, parts, part):
    rows = values.shape[0] // parts
    return lax.dynamic_slice_in_dim(values, part * rows, rows, axis=0)


def rounded_sum(left, right):
    total = left.astype(jnp.float32) + right.astype(jnp.float32)
    return total.astype(jnp.bfloat16)


def fits_square(tokens, up_weight):
    shares = lax.axis_size("group")
    rows, features = tokens.shape
    return (
        lax.axis_size("dp") == 4
        and shares == 8
        and rows % (32 * shares) == 0
        and up_weight.shape[0] * 4 == features
        and up_weight.shape[0] % 256 == 0
        and up_weight.shape[1] % 256 == 0
    )


def flipped(index, mask, size):
    out, bit = index, 1
    while bit < size:
        out = out + bit * ((mask // bit) % 2) * (1 - 2 * ((index // bit) % 2))
        bit *= 2
    return out


def line_orders(chips):
    return [sorted(range(chips), key=lambda w: (abs(w - c), w)) for c in range(chips)]


def gelu_parts(pre, d_act):
    scale, cubic = 0.7978845608028654, 0.044715
    square = pre * pre
    wave = jnp.tanh(scale * (pre + cubic * (square * pre)))
    half = 0.5 * (1.0 + wave)
    slope = half + 0.5 * pre * (1.0 - wave * wave) * (scale * (1.0 + 3.0 * cubic * square))
    return pre * half, d_act * slope


def scratch(shares, rows, cols, units, flat, types):
    half, bf16, f32 = rows // 2, jnp.bfloat16, jnp.float32
    dma = pltpu.SemaphoreType.DMA
    return {
        "feats": pltpu.VMEM((2, shares, 4, rows, cols), bf16),
        "weights": pltpu.VMEM((2, cols, units), bf16),
        "lines": pltpu.VMEM((4, shares * rows, cols), bf16),
        "packed": pltpu.VMEM((4, rows, cols), bf16),
        "slot": pltpu.VMEM((1, shares * rows), jnp.int32),
        "counts": pltpu.VMEM((4, 8, 128), f32),
        "own": pltpu.VMEM((shares * rows, cols), bf16),
        "staged": pltpu.VMEM((2, 4, rows, cols), bf16),
        "far_x": pltpu.VMEM((shares, 2, 2, half, units), bf16),
        "far_y": pltpu.VMEM((shares, 2, 2, half, units), bf16),
        "kept": pltpu.VMEM((shares, 2, rows, units), bf16),
        "mid_x": pltpu.VMEM((shares, 2, half, units), bf16),
        "mid_y": pltpu.VMEM((shares, 2, half, units), bf16),
        "got_x": pltpu.VMEM((shares, 2, 2, half, units), bf16),
        "got_y": pltpu.VMEM((shares, 2, 2, half, units), bf16),
        "last_x": pltpu.VMEM((shares, 2, half, units), bf16),
        "last_y": pltpu.VMEM((shares, 2, half, units), bf16),
        "snap_out": pltpu.VMEM((shares, 3, 1, flat), f32),
        "mask": pltpu.VMEM((1, shares * rows), jnp.int32),
        "held_params": pltpu.VMEM((shares, flat), types[0]),
        "held_first": pltpu.VMEM((shares, flat), types[1]),
        "held_second": pltpu.VMEM((shares, flat), types[2]),
        "writer": pltpu.SMEM((shares,), jnp.int32),
        "small_sem": dma((5,)),
        "line_sem": dma((4,)),
        "own_sem": dma((1,)),
        "count_send": dma((4,)),
        "count_got": dma((4,)),
        "weight_sem": dma((2,)),
        "cross_send": dma((2, 4)),
        "cross_got": dma((2, 4)),
        "line_send": dma((2, 2, shares // 2)),
        "twin_send": dma((2, shares)),
        "feat_got": dma((2, shares)),
        "far_send": dma((2, 2, shares)),
        "far_got": dma((2, 2, shares)),
        "last_send": dma((2, shares)),
        "last_got": dma((2, shares)),
        "wide_send": dma((2, shares)),
        "wide_got": dma((2, shares)),
        "over_send": dma((2, shares)),
        "over_got": dma((2, shares)),
        "snap_send": dma((shares,)),
        "snap_got": dma((shares,)),
    }


def step_kernel(names, shares, used, *refs):
    tokens, cotangent, up_weight, down_weight, *small = refs[:9]
    *total, last_feats, wide, snap_in, most = refs[9:15]
    s = dict(zip(names, refs[15:]))
    feats, weights, mask, writer = s["feats"], s["weights"], s["mask"], s["writer"]
    held = [s["held_params"], s["held_first"], s["held_second"]]
    me, group = lax.axis_index("dp"), lax.axis_index("group")
    square = [me, me + 1 - 2 * (me % 2), me + 2 - 4 * (me // 2), 3 - me]
    twin = flipped(group, 1, shares)
    chip, core = group // 2, group % 2
    orders = line_orders(shares // 2)
    inner = range(1, len(orders) - 1)
    outer = (0, len(orders) - 1)
    table = sum(w << (8 * c + 2 * p) for c, order in enumerate(orders) for p, w in enumerate(order))
    own_order = table // ((1 + 255 * (chip % 2)) * (1 + 65535 * (chip // 2))) % 256
    rows, cols, units = feats.shape[3], feats.shape[4], weights.shape[2]
    half, tile = rows // 2, 256
    bf16, f32 = jnp.bfloat16, jnp.float32
    top, low = pl.ds(0, half), pl.ds(half, half)

    def send(src, dst, send_sem, got_sem, dp_to, group_to):
        return pltpu.make_async_remote_copy(
            src_ref=src,
            dst_ref=dst,
            send_sem=send_sem,
            recv_sem=got_sem,
            device_id=(dp_to, group_to),
            device_id_type=pl.DeviceIdType.MESH,
        )

    barrier = pltpu.get_barrier_semaphore()
    partners = [(d, group) for d in square[1:]]
    partners += [(me, flipped(group, k, shares)) for k in range(1, shares)]
    for there in partners:
        pl.semaphore_signal(
            barrier, inc=1, device_id=there, device_id_type=pl.DeviceIdType.MESH
        )

    def owner_of(k):
        place = k // 2
        there = own_order // ((1 + 3 * (place % 2)) * (1 + 15 * (place // 2))) % 4
        return 2 * there + (core + k) % 2

    def in_use(k):
        return owner_of(k) < used

    def columns_of(r):
        return pl.ds(pl.multiple_of(square[r] * cols, cols), cols)

    def load_lines(source, r):
        return pltpu.make_async_copy(
            source.at[:, columns_of(r)], s["lines"].at[r], s["line_sem"].at[r]
        )

    load_own = pltpu.make_async_copy(
        cotangent.at[:, columns_of(0)], s["own"], s["own_sem"].at[0]
    )
    load_weights = [
        pltpu.make_async_copy(w, weights.at[t], s["weight_sem"].at[t])
        for t, w in enumerate((up_weight, down_weight))
    ]
    load_small = [
        pltpu.make_async_copy(src, dst, s["small_sem"].at[n])
        for n, (src, dst) in enumerate(zip(small, [mask] + held + [writer]))
    ]
    load_small[0].start()
    for r in (3, 1, 2, 0):
        load_lines(cotangent, r).start()
    for copy in load_small[1:]:
        copy.start()

    def rows_to_slots():
        load_small[0].wait()
        count = mask.shape[1]
        row = lax.broadcasted_iota(jnp.int32, (count, count), 0)
        column = lax.broadcasted_iota(jnp.int32, (count, count), 1)
        before = jnp.where(row < column, 1.0, 0.0).astype(bf16)
        ones = jnp.broadcast_to(mask[...].astype(f32), (8, count))
        places = matmul(ones.astype(bf16), before)[:1].astype(jnp.int32)
        s["slot"][...] = jnp.where(mask[...] > 0, places, -1)
        held_here = jnp.sum(ones, axis=1, keepdims=True)
        s["counts"][0] = jnp.broadcast_to(held_here, (8, 128))

    def picker(k):
        shape = (rows, mask.shape[1])
        at = lax.broadcasted_iota(jnp.int32, shape, 0) + owner_of(k) * rows
        return jnp.where(at == s["slot"][...], 1.0, 0.0).astype(bf16)

    def pick(chosen, source, store):
        def some(m, carry):
            here = pl.ds(pl.multiple_of(m * tile, tile), tile)
            store(here, matmul(chosen, source[:, here]).astype(bf16))
            return carry

        lax.fori_loop(0, cols // tile, some, 0)

    def normal_rows(chosen, parts, store):
        for r in range(4):

            def keep(here, values):
                s["packed"][r, :, here] = values

            pick(chosen, s["lines"].at[r], keep)
        step = 16

        def some(i, carry):
            here = pl.ds(pl.multiple_of(i * step, step), step)
            values = [s["packed"][r, here].astype(f32) for r in range(4)]
            mean = sum(jnp.sum(v, axis=1, keepdims=True) for v in values) / (4 * cols)
            centred = [v - mean for v in values]
            squares = sum(jnp.sum(c * c, axis=1, keepdims=True) for c in centred)
            scale = lax.rsqrt(squares / (4 * cols) + EPS)
            for r in range(parts):
                store(r, here, (centred[r] * scale).astype(bf16))
            return carry

        lax.fori_loop(0, rows // step, some, 0)

    def cross(t, r):
        return send(
            s["staged"].at[t, r],
            feats.at[t, 0, r],
            s["cross_send"].at[t, r],
            s["cross_got"].at[t, r],
            square[r],
            group,
        )

    def counted(r):
        return send(
            s["counts"].at[0],
            s["counts"].at[r],
            s["count_send"].at[r],
            s["count_got"].at[r],
            square[r],
            group,
        )

    def store_staged(r, here, values):
        s["staged"][0, r, here] = values

    rows_to_slots()
    chosen = picker(0)
    for n, r in enumerate((3, 1, 2, 0)):
        load_lines(cotangent, r).wait()

        def keep(here, values):
            s["staged"][1, r, :, here] = values

        pick(chosen, s["lines"].at[r], keep)
        load_lines(tokens, r).start()
        if n == 0:
            pl.semaphore_wait(barrier, len(partners))
        if r:

            @pl.when(in_use(0))
            def _():
                cross(1, r).start()

    for copy in load_weights:
        copy.start()
    load_own.start()
    for r in range(4):
        load_lines(tokens, r).wait()
    normal_rows(chosen, 4, store_staged)
    for r in (3, 1, 2):

        @pl.when(in_use(0))
        def _():
            cross(0, r).start()

        counted(r).start()

    for copy in load_small[1:]:
        copy.wait()
    held = [ref[...].astype(f32) for ref in held]
    for w in range(shares):
        for j in range(3):
            picked = jnp.zeros((1, held[j].shape[1]), f32)
            for source in range(shares):
                picked = jnp.where(writer[w] == source, held[j][source : source + 1], picked)
            s["snap_out"][w, j] = picked

    def regrouped(k):
        return send(
            s["snap_out"].at[flipped(group, k, shares)],
            snap_in.at[group],
            s["snap_send"].at[k],
            s["snap_got"].at[k],
            me,
            flipped(group, k, shares),
        )

    for k in range(1, shares):
        regrouped(k).start()
    snap_in[group] = s["snap_out"][group]

    def onward(t, c, w, way):
        place, there = orders[c].index(w), orders[c + way].index(w)
        return send(
            feats.at[t, 2 * place, pl.ds(1, 3)],
            feats.at[t, 2 * there, pl.ds(1, 3)],
            s["line_send"].at[t, (way + 1) // 2, place],
            s["feat_got"].at[t, 2 * there],
            me,
            group + 2 * way,
        )

    def moves(c, place):
        w = orders[c][place]
        ways = [way for way, goes in ((-1, w >= c), (1, w <= c)) if goes]
        return [(w, way) for way in ways if 0 <= c + way < len(orders)]

    def move_on(t, chips, place):
        for c in chips:

            @pl.when(chip == c)
            def _():
                for w, way in moves(c, place):

                    @pl.when(2 * w + core < used)
                    def _():
                        onward(t, c, w, way).start()

    def arrived(t, k):
        @pl.when(in_use(k))
        def _():
            to_twin(t, k - 1).wait_recv()

    def to_twin(t, k):
        return send(
            feats.at[t, k, pl.ds(1, 3)],
            feats.at[t, k + 1, pl.ds(1, 3)],
            s["twin_send"].at[t, k],
            s["feat_got"].at[t, k + 1],
            me,
            twin,
        )

    def start_total(m, carry):
        here = pl.ds(pl.multiple_of(m * tile, tile), tile)
        for t in range(2):
            total[t][here] = jnp.zeros((tile, units), f32)
        return carry

    lax.fori_loop(0, cols // tile, start_total, 0)
    load_own.wait()
    def far(t, axis, k):
        pair = (s["far_x"], s["got_x"]) if axis == 0 else (s["far_y"], s["got_y"])
        return send(
            pair[0].at[k, t],
            pair[1].at[k, t],
            s["far_send"].at[axis, t, k],
            s["far_got"].at[axis, t, k],
            square[1 + axis],
            group,
        )

    def last(axis, k):
        pair = (s["mid_y"], s["last_x"]) if axis == 0 else (s["mid_x"], s["last_y"])
        return send(
            pair[0].at[k],
            pair[1].at[k],
            s["last_send"].at[axis, k],
            s["last_got"].at[axis, k],
            square[1 + axis],
            group,
        )

    def spread(axis, k):
        return send(
            wide.at[k, :, 0],
            wide.at[k, :, 1 + axis],
            s["wide_send"].at[axis, k],
            s["wide_got"].at[axis, k],
            square[1 + axis],
            group,
        )

    def over(axis, k):
        here = low if axis == 0 else top
        return send(
            wide.at[k, :, 2 - axis, here],
            wide.at[k, :, 3, here],
            s["over_send"].at[axis, k],
            s["over_got"].at[axis, k],
            square[1 + axis],
            group,
        )

    def products(t, k):
        def column(i, carry):
            here = pl.ds(pl.multiple_of(i * tile, tile), tile)
            left = feats[t, k, pl.ds(1, 3)].reshape(3 * rows, cols)
            out = matmul(left, weights[t, :, here]).astype(bf16)
            part = [None] + [out[r * rows : (r + 1) * rows] for r in range(3)]
            s["far_x"][k, t, 0, :, here] = part[3][:half]
            s["far_x"][k, t, 1, :, here] = part[1][:half]
            s["far_y"][k, t, 0, :, here] = part[3][half:]
            s["far_y"][k, t, 1, :, here] = part[2][half:]
            s["mid_x"][k, t, :, here] = part[2][:half]
            s["mid_y"][k, t, :, here] = part[1][half:]
            return carry

        lax.fori_loop(0, units // tile, column, 0)
        far(t, 0, k).start()
        far(t, 1, k).start()


    def stage_products(k):
        at_end = (chip == outer[0]) | (chip == outer[1])
        within = jnp.logical_not(at_end)
        for t in (1, 0):

            @pl.when(k == 0)
            def _():
                load_weights[t].wait()

            @pl.when((k == 0) & in_use(0))
            def _():
                for r in (1, 2, 3):
                    cross(t, r).wait_recv()
                move_on(t, range(len(orders)), 0)

            @pl.when(k % 2 == 1)
            def _():
                arrived(t, k)

            @pl.when(k == 2)
            def _():
                arrived(t, 2)
                move_on(t, inner, 1)

            @pl.when((k == 2) & within)
            def _():
                arrived(t, 4)
                move_on(t, inner, 2)

            @pl.when((k == 4) & within)
            def _():
                arrived(t, 6)
                move_on(t, inner, 3)

            @pl.when((k >= 4) & (k % 2 == 0) & at_end)
            def _():
                arrived(t, k)

            @pl.when((k % 2 == 0) & in_use(k))
            def _():
                to_twin(t, k).start()

            @pl.when(in_use(k))
            def _():
                products(t, k)

            @pl.when((k == shares - 1) & jnp.logical_not(in_use(k)))
            def _():
                last_feats[t] = jnp.zeros(last_feats.shape[1:], bf16)
                wide[k, t] = jnp.zeros(wide.shape[2:], bf16)

    def own_rows(k):
        chosen = picker(k)

        def store_normed(r, here, values):
            feats[0, k, r, here] = values

        def store_masked(here, values):
            feats[1, k, 0, :, here] = values

        normal_rows(chosen, 1, store_normed)
        pick(chosen, s["own"], store_masked)

    def stage_own(k):
        @pl.when(k == 0)
        def _():
            for t in range(2):
                feats[t, 0, 0] = s["staged"][t, 0]

        @pl.when(k > 0)
        def _():
            own_rows(k)

        for t in range(2):

            def column(i, carry):
                here = pl.ds(pl.multiple_of(i * tile, tile), tile)
                out = matmul(feats[t, k, 0], weights[t, :, here])
                s["kept"][k, t, :, here] = out.astype(bf16)
                return carry

            lax.fori_loop(0, units // tile, column, 0)

            @pl.when(k == shares - 1)
            def _():
                for m in range(cols // tile):
                    here = pl.ds(m * tile, tile)
                    last_feats[t, here] = feats[t, k, :, :, here].reshape(4 * rows, tile).T

    def stage_middle(k):
        for t in range(2):
            far(t, 0, k).wait_recv()
            s["mid_x"][k, t] = rounded_sum(s["mid_x"][k, t], s["got_x"][k, t, 0])
        last(1, k).start()
        for t in range(2):
            far(t, 1, k).wait_recv()
            s["mid_y"][k, t] = rounded_sum(s["mid_y"][k, t], s["got_y"][k, t, 0])
        last(0, k).start()

    def stage_gelu(k):
        last(1, k).wait_recv()
        last(0, k).wait_recv()
        step = 16
        for axis, near_ref, last_ref in (
            (0, s["got_x"], s["last_y"]),
            (1, s["got_y"], s["last_x"]),
        ):

            def some(i, carry):
                here = pl.ds(pl.multiple_of(i * step, step), step)
                out = pl.ds(pl.multiple_of(axis * half + i * step, step), step)
                sums = [
                    s["kept"][k, t, out].astype(f32)
                    + near_ref[k, t, 1, here].astype(f32)
                    + last_ref[k, t, here].astype(f32)
                    for t in range(2)
                ]
                act, grad_pre = gelu_parts(*sums)
                wide[k, 0, 0, out] = grad_pre.astype(bf16)
                wide[k, 1, 0, out] = act.astype(bf16)
                return carry

            lax.fori_loop(0, half // step, some, 0)
        spread(0, k).start()
        spread(1, k).start()

    def stage_over(k):
        spread(0, k).wait_recv()
        over(1, k).start()
        spread(1, k).wait_recv()
        over(0, k).start()

    def stage_gradient(k):
        over(0, k).wait_recv()
        over(1, k).wait_recv()

        @pl.when(k < shares - 1)
        def _():
            for t in range(2):

                def some(m, carry):
                    here = pl.ds(pl.multiple_of(m * tile, tile), tile)
                    left = feats[t, k, :, :, here].reshape(4 * rows, tile)
                    right = wide[k, t].reshape(4 * rows, units)
                    total[t][here] = total[t][here] + outer_sum(left, right)
                    return carry

                lax.fori_loop(0, cols // tile, some, 0)

    def when_used(stage):
        def guarded(k):
            @pl.when(in_use(k))
            def _():
                stage(k)

        return guarded

    stages = [stage_middle, stage_gelu, stage_over, stage_gradient]
    stages = [stage_products] + [when_used(stage) for stage in stages]
    lags = list(enumerate(stages))
    lags = [lags[1], lags[0]] + lags[2:4] + [(0, when_used(stage_own)), lags[4]]

    def pipeline(step, carry):
        for lag, stage in lags:

            @pl.when((step >= lag) & (step - lag < shares))
            def _():
                stage(step - lag)

        return carry

    lax.fori_loop(0, shares + len(stages) - 1, pipeline, 0)

    for k in range(1, shares):
        regrouped(k).wait()
    most[...] = s["counts"][0]
    for r in (1, 2, 3):
        counted(r).wait()
        most[...] = jnp.maximum(most[...], s["counts"][r])
    for t in range(2):

        @pl.when(in_use(0))
        def _():
            for r in (1, 2, 3):
                cross(t, r).wait_send()

        for k in range(0, shares, 2):

            @pl.when(in_use(k))
            def _():
                to_twin(t, k).wait_send()

    for c in range(len(orders)):

        @pl.when(chip == c)
        def _():
            for place in range(len(orders)):
                for w, way in moves(c, place):

                    @pl.when(2 * w + core < used)
                    def _():
                        for t in range(2):
                            onward(t, c, w, way).wait_send()

    def finish(k, carry):
        @pl.when(in_use(k))
        def _():
            for axis in range(2):
                for t in range(2):
                    far(t, axis, k).wait_send()
                last(axis, k).wait_send()
                spread(axis, k).wait_send()
                over(axis, k).wait_send()

        return carry

    lax.fori_loop(0, shares, finish, 0)


def last_kernel(
    total_up,
    total_down,
    feats,
    wide,
    snap,
    grad_up,
    grad_down,
    params,
    moments,
    ready,
    params_ready,
    moments_ready,
    sem,
    snap_sem,
):
    shares, rows, units = wide.shape[0], wide.shape[3], wide.shape[4]
    slots, tile = ready.shape[0], ready.shape[1]
    tiles = total_up.shape[0] // tile
    width = params.shape[1] // shares
    for source in range(shares):
        here = pl.ds(source * width, width)
        params_ready[:, here] = snap[source, 0].astype(params.dtype)
        for j in range(2):
            moments_ready[j, :, here] = snap[source, 1 + j]
    small = [
        pltpu.make_async_copy(params_ready, params, snap_sem.at[0]),
        pltpu.make_async_copy(moments_ready, moments, snap_sem.at[1]),
    ]
    for copy in small:
        copy.start()

    def written(n):
        t, m = n // tiles, n % tiles
        return pltpu.make_async_copy(
            ready.at[n % slots],
            (grad_up, grad_down)[t].at[pl.ds(m * tile, tile)],
            sem.at[n % slots],
        )

    for n in range(2 * tiles):
        t, here = n // tiles, pl.ds(n % tiles * tile, tile)
        if n >= slots:
            written(n - slots).wait()
        right = wide[shares - 1, t].reshape(4 * rows, units)
        ready[n % slots] = (total_up, total_down)[t][here] + matmul(feats[t, here], right)
        written(n).start()
    for n in range(max(0, 2 * tiles - slots), 2 * tiles):
        written(n).wait()
    for copy in small:
        copy.wait()


def weight_gradients(
    tokens,
    frame_mask,
    cotangent,
    up_weight,
    down_weight,
    snap_params,
    first_moment,
    second_moment,
    range_of_writer,
):
    shares = lax.axis_size("group")
    rows, (cols, units), flat = tokens.shape[0] // shares, up_weight.shape, snap_params.shape[1]
    types = [x.dtype for x in (snap_params, first_moment, second_moment)]
    buffers = scratch(shares, rows, cols, units, flat, types)
    anywhere = pl.BlockSpec(memory_space=pl.ANY)
    inside = pl.BlockSpec(memory_space=pltpu.VMEM)
    bf16, f32 = jnp.bfloat16, jnp.float32
    piece_flops = 8 * 4 * rows * cols * units

    def step(used):
        return pl.pallas_call(
            functools.partial(step_kernel, tuple(buffers), shares, used),
            out_shape=(
                pltpu.VMEM((cols, units), f32),
                pltpu.VMEM((cols, units), f32),
                pltpu.VMEM((2, cols, 4 * rows), bf16),
                pltpu.VMEM((shares, 2, 4, rows, units), bf16),
                pltpu.VMEM((shares, 3, 1, flat), f32),
                pltpu.VMEM((8, 128), f32),
            ),
            in_specs=[anywhere] * 9,
            out_specs=(inside,) * 6,
            scratch_shapes=list(buffers.values()),
            compiler_params=pltpu.CompilerParams(
                collective_id=shares - used, has_side_effects=True, vmem_limit_bytes=STEP_VMEM
            ),
            cost_estimate=pl.CostEstimate(
                flops=used * piece_flops,
                bytes_accessed=4 * cols * units + 4 * tokens.size,
                transcendentals=used * rows * units,
            ),
            name=f"backward_step_{used}",
        )(
            tokens,
            cotangent,
            up_weight,
            down_weight,
            frame_mask[None, :],
            snap_params,
            first_moment,
            second_moment,
            range_of_writer,
        )

    def finish(*sums):
        tile, slots = 256, 4
        return pl.pallas_call(
            last_kernel,
            out_shape=(
                jax.ShapeDtypeStruct((cols, units), f32),
                jax.ShapeDtypeStruct((cols, units), f32),
                jax.ShapeDtypeStruct((1, shares * flat), snap_params.dtype),
                jax.ShapeDtypeStruct((2, 1, shares * flat), first_moment.dtype),
            ),
            in_specs=[inside] * 5,
            out_specs=(anywhere,) * 4,
            scratch_shapes=[
                pltpu.VMEM((slots, tile, units), f32),
                pltpu.VMEM((1, shares * flat), snap_params.dtype),
                pltpu.VMEM((2, 1, shares * flat), first_moment.dtype),
                pltpu.SemaphoreType.DMA((slots,)),
                pltpu.SemaphoreType.DMA((2,)),
            ],
            compiler_params=pltpu.CompilerParams(vmem_limit_bytes=LAST_VMEM),
            cost_estimate=pl.CostEstimate(
                flops=piece_flops // 2, bytes_accessed=8 * cols * units, transcendentals=0
            ),
            name="last_piece",
        )(*sums)

    fewer = shares - 1
    *sums, most = step(fewer)
    results = finish(*sums)
    return lax.cond(
        most[0, 0] > fewer * rows, lambda done: finish(*step(shares)[:5]), lambda done: done, results
    )


def weight_gradients_any(tokens, frame_mask, cotangent, up_weight, down_weight, *snapshot):
    shares = lax.axis_size("group")
    group = lax.axis_index("group")
    mask = own_part(frame_mask, shares, group)[:, None].astype(jnp.bfloat16)

    def to_features(rows_here):
        part = lax.all_to_all(rows_here, "dp", split_axis=1, concat_axis=0, tiled=True)
        return lax.all_gather(part, "group", axis=0, tiled=True)

    def own_rows_total(left, weight):
        part = matmul(left, weight).astype(jnp.bfloat16)
        return lax.psum_scatter(part, "dp", scatter_dimension=0, tiled=True).astype(jnp.float32)

    normed = to_features(normalize(own_part(tokens, shares, group)))
    masked = to_features(own_part(cotangent, shares, group) * mask)
    act, grad_pre = gelu_pair(
        own_rows_total(normed, up_weight), own_rows_total(masked, down_weight)
    )
    grad_down = outer_sum(masked, lax.all_gather(act, "dp", axis=0, tiled=True))
    grad_up = outer_sum(normed, lax.all_gather(grad_pre, "dp", axis=0, tiled=True))
    return grad_up, grad_down, *regroup(*snapshot)


def per_device(
    tokens,
    frame_mask,
    cotangent,
    up_weight,
    down_weight,
    snap_params,
    first_moment,
    second_moment,
    range_of_writer,
):
    square = fits_square(tokens, up_weight)
    compute = weight_gradients if square else weight_gradients_any
    snapshot = (snap_params, first_moment, second_moment, range_of_writer)
    return compute(tokens, frame_mask, cotangent, up_weight, down_weight, *snapshot)


def solution(mesh):
    placed = (
        P("dp", None),
        P("dp"),
        P("dp", None),
        P("dp", "group"),
        P("dp", "group"),
        P(None, ("dp", "group")),
        P(None, ("dp", "group")),
        P(None, ("dp", "group")),
        P(),
    )
    return jax.shard_map(
        per_device,
        mesh=mesh,
        in_specs=placed,
        out_specs=(P("dp", "group"), P("dp", "group"), P("group", "dp"), P(None, "group", "dp")),
        check_vma=False,
    )
```

```python
import functools

import jax
import jax.numpy as jnp
from jax import lax
from jax.experimental import pallas as pl
from jax.experimental.pallas import tpu as pltpu
from jax.sharding import PartitionSpec as P

EPS = 1e-06
STEP_VMEM, LAST_VMEM = 41 * 2**20, 8 * 2**20


def normalize(tokens):
    values = tokens.astype(jnp.float32)
    centred = values - jnp.mean(values, axis=1, keepdims=True)
    spread = jnp.mean(centred * centred, axis=1, keepdims=True)
    return (centred * lax.rsqrt(spread + EPS)).astype(jnp.bfloat16)


def gelu_pair(pre, d_act):
    act, pullback = jax.vjp(lambda v: jax.nn.gelu(v, approximate=True), pre)
    return (act.astype(jnp.bfloat16), pullback(d_act)[0].astype(jnp.bfloat16))


def outer_sum(left, right):
    return lax.dot_general(
        left, right, (((0,), (0,)), ((), ())), preferred_element_type=jnp.float32
    )


def regroup(snap_params, first_moment, second_moment, range_of_writer):
    flat = snap_params.shape[1]
    held = jnp.concatenate(
        [snap_params, first_moment.astype(jnp.bfloat16), second_moment.astype(jnp.bfloat16)],
        axis=1,
    )
    send = jnp.take(held, range_of_writer, axis=0).reshape(-1, 3, flat)
    got = lax.all_to_all(send, "group", split_axis=0, concat_axis=0, tiled=True)
    lines = jnp.swapaxes(got, 0, 1).reshape(3, 1, -1)
    return lines[0], lines[1:].astype(first_moment.dtype)


def matmul(left, right):
    return jnp.dot(left, right, preferred_element_type=jnp.float32)


def own_part(values, parts, part):
    rows = values.shape[0] // parts
    return lax.dynamic_slice_in_dim(values, part * rows, rows, axis=0)


def rounded_sum(left, right):
    total = left.astype(jnp.float32) + right.astype(jnp.float32)
    return total.astype(jnp.bfloat16)


def fits_square(tokens, up_weight):
    shares = lax.axis_size("group")
    rows, features = tokens.shape
    return (
        lax.axis_size("dp") == 4
        and shares == 8
        and rows % (32 * shares) == 0
        and up_weight.shape[0] * 4 == features
        and up_weight.shape[0] % 256 == 0
        and up_weight.shape[1] % 256 == 0
    )


def flipped(index, mask, size):
    out, bit = index, 1
    while bit < size:
        out = out + bit * ((mask // bit) % 2) * (1 - 2 * ((index // bit) % 2))
        bit *= 2
    return out


def line_orders(chips):
    return [sorted(range(chips), key=lambda w: (abs(w - c), w)) for c in range(chips)]


def gelu_parts(pre, d_act):
    scale, cubic = 0.7978845608028654, 0.044715
    square = pre * pre
    wave = jnp.tanh(scale * (pre + cubic * (square * pre)))
    half = 0.5 * (1.0 + wave)
    slope = half + 0.5 * pre * (1.0 - wave * wave) * (scale * (1.0 + 3.0 * cubic * square))
    return pre * half, d_act * slope


def scratch(shares, rows, cols, units, flat, types):
    half, bf16, f32 = rows // 2, jnp.bfloat16, jnp.float32
    dma = pltpu.SemaphoreType.DMA
    return {
        "feats": pltpu.VMEM((2, shares, 4, rows, cols), bf16),
        "weights": pltpu.VMEM((2, cols, units), bf16),
        "lines": pltpu.VMEM((4, shares * rows, cols), bf16),
        "packed": pltpu.VMEM((4, rows, cols), bf16),
        "slot": pltpu.VMEM((1, shares * rows), jnp.int32),
        "counts": pltpu.VMEM((4, 8, 128), f32),
        "own": pltpu.VMEM((shares * rows, cols), bf16),
        "staged": pltpu.VMEM((2, 4, rows, cols), bf16),
        "far_x": pltpu.VMEM((shares, 2, 2, half, units), bf16),
        "far_y": pltpu.VMEM((shares, 2, 2, half, units), bf16),
        "kept": pltpu.VMEM((shares, 2, rows, units), bf16),
        "mid_x": pltpu.VMEM((shares, 2, half, units), bf16),
        "mid_y": pltpu.VMEM((shares, 2, half, units), bf16),
        "got_x": pltpu.VMEM((shares, 2, 2, half, units), bf16),
        "got_y": pltpu.VMEM((shares, 2, 2, half, units), bf16),
        "last_x": pltpu.VMEM((shares, 2, half, units), bf16),
        "last_y": pltpu.VMEM((shares, 2, half, units), bf16),
        "snap_out": pltpu.VMEM((shares, 3, 1, flat), f32),
        "mask": pltpu.VMEM((1, shares * rows), jnp.int32),
        "held_params": pltpu.VMEM((shares, flat), types[0]),
        "held_first": pltpu.VMEM((shares, flat), types[1]),
        "held_second": pltpu.VMEM((shares, flat), types[2]),
        "writer": pltpu.SMEM((shares,), jnp.int32),
        "small_sem": dma((5,)),
        "line_sem": dma((4,)),
        "own_sem": dma((1,)),
        "count_send": dma((4,)),
        "count_got": dma((4,)),
        "weight_sem": dma((2,)),
        "cross_send": dma((2, 4)),
        "cross_got": dma((2, 4)),
        "line_send": dma((2, 2, shares // 2)),
        "twin_send": dma((2, shares)),
        "feat_got": dma((2, shares)),
        "far_send": dma((2, 2, shares)),
        "far_got": dma((2, 2, shares)),
        "last_send": dma((2, shares)),
        "last_got": dma((2, shares)),
        "wide_send": dma((2, shares)),
        "wide_got": dma((2, shares)),
        "over_send": dma((2, shares)),
        "over_got": dma((2, shares)),
        "snap_send": dma((shares,)),
        "snap_got": dma((shares,)),
    }


def step_kernel(names, shares, used, *refs):
    tokens, cotangent, up_weight, down_weight, *small = refs[:9]
    *total, last_feats, wide, snap_in, most = refs[9:15]
    s = dict(zip(names, refs[15:]))
    feats, weights, mask, writer = s["feats"], s["weights"], s["mask"], s["writer"]
    held = [s["held_params"], s["held_first"], s["held_second"]]
    me, group = lax.axis_index("dp"), lax.axis_index("group")
    square = [me, me + 1 - 2 * (me % 2), me + 2 - 4 * (me // 2), 3 - me]
    twin = flipped(group, 1, shares)
    chip, core = group // 2, group % 2
    orders = line_orders(shares // 2)
    inner = range(1, len(orders) - 1)
    outer = (0, len(orders) - 1)
    table = sum(w << (8 * c + 2 * p) for c, order in enumerate(orders) for p, w in enumerate(order))
    own_order = table // ((1 + 255 * (chip % 2)) * (1 + 65535 * (chip // 2))) % 256
    rows, cols, units = feats.shape[3], feats.shape[4], weights.shape[2]
    half, tile = rows // 2, 256
    bf16, f32 = jnp.bfloat16, jnp.float32
    top, low = pl.ds(0, half), pl.ds(half, half)

    def send(src, dst, send_sem, got_sem, dp_to, group_to):
        return pltpu.make_async_remote_copy(
            src_ref=src,
            dst_ref=dst,
            send_sem=send_sem,
            recv_sem=got_sem,
            device_id=(dp_to, group_to),
            device_id_type=pl.DeviceIdType.MESH,
        )

    barrier = pltpu.get_barrier_semaphore()
    partners = [(d, group) for d in square[1:]]
    partners += [(me, flipped(group, k, shares)) for k in range(1, shares)]
    for there in partners:
        pl.semaphore_signal(
            barrier, inc=1, device_id=there, device_id_type=pl.DeviceIdType.MESH
        )

    def owner_of(k):
        place = k // 2
        there = own_order // ((1 + 3 * (place % 2)) * (1 + 15 * (place // 2))) % 4
        return 2 * there + (core + k) % 2

    def in_use(k):
        return owner_of(k) < used

    def columns_of(r):
        return pl.ds(pl.multiple_of(square[r] * cols, cols), cols)

    def load_lines(source, r):
        return pltpu.make_async_copy(
            source.at[:, columns_of(r)], s["lines"].at[r], s["line_sem"].at[r]
        )

    load_own = pltpu.make_async_copy(
        cotangent.at[:, columns_of(0)], s["own"], s["own_sem"].at[0]
    )
    load_weights = [
        pltpu.make_async_copy(w, weights.at[t], s["weight_sem"].at[t])
        for t, w in enumerate((up_weight, down_weight))
    ]
    load_small = [
        pltpu.make_async_copy(src, dst, s["small_sem"].at[n])
        for n, (src, dst) in enumerate(zip(small, [mask] + held + [writer]))
    ]
    load_small[0].start()
    for r in (3, 1, 2, 0):
        load_lines(cotangent, r).start()
    for copy in load_small[1:]:
        copy.start()

    def rows_to_slots():
        load_small[0].wait()
        count = mask.shape[1]
        row = lax.broadcasted_iota(jnp.int32, (count, count), 0)
        column = lax.broadcasted_iota(jnp.int32, (count, count), 1)
        before = jnp.where(row < column, 1.0, 0.0).astype(bf16)
        ones = jnp.broadcast_to(mask[...].astype(f32), (8, count))
        places = matmul(ones.astype(bf16), before)[:1].astype(jnp.int32)
        s["slot"][...] = jnp.where(mask[...] > 0, places, -1)
        held_here = jnp.sum(ones, axis=1, keepdims=True)
        s["counts"][0] = jnp.broadcast_to(held_here, (8, 128))

    def picker(k):
        shape = (rows, mask.shape[1])
        at = lax.broadcasted_iota(jnp.int32, shape, 0) + owner_of(k) * rows
        return jnp.where(at == s["slot"][...], 1.0, 0.0).astype(bf16)

    def pick(chosen, source, store):
        store(pl.ds(0, cols), matmul(chosen, source[...]).astype(bf16))

    def normal_rows(chosen, parts, store):
        for r in range(4):

            def keep(here, values):
                s["packed"][r, :, here] = values

            pick(chosen, s["lines"].at[r], keep)
        step = 16

        def some(i, carry):
            here = pl.ds(pl.multiple_of(i * step, step), step)
            values = [s["packed"][r, here].astype(f32) for r in range(4)]
            mean = sum(jnp.sum(v, axis=1, keepdims=True) for v in values) / (4 * cols)
            centred = [v - mean for v in values]
            squares = sum(jnp.sum(c * c, axis=1, keepdims=True) for c in centred)
            scale = lax.rsqrt(squares / (4 * cols) + EPS)
            for r in range(parts):
                store(r, here, (centred[r] * scale).astype(bf16))
            return carry

        lax.fori_loop(0, rows // step, some, 0)

    def cross(t, r):
        return send(
            s["staged"].at[t, r],
            feats.at[t, 0, r],
            s["cross_send"].at[t, r],
            s["cross_got"].at[t, r],
            square[r],
            group,
        )

    def counted(r):
        return send(
            s["counts"].at[0],
            s["counts"].at[r],
            s["count_send"].at[r],
            s["count_got"].at[r],
            square[r],
            group,
        )

    def store_staged(r, here, values):
        s["staged"][0, r, here] = values

    rows_to_slots()
    chosen = picker(0)
    for n, r in enumerate((3, 1, 2, 0)):
        load_lines(cotangent, r).wait()

        def keep(here, values):
            s["staged"][1, r, :, here] = values

        pick(chosen, s["lines"].at[r], keep)
        load_lines(tokens, r).start()
        if n == 0:
            pl.semaphore_wait(barrier, len(partners))
        if r:

            @pl.when(in_use(0))
            def _():
                cross(1, r).start()

    for copy in load_weights:
        copy.start()
    load_own.start()
    for r in range(4):
        load_lines(tokens, r).wait()
    normal_rows(chosen, 4, store_staged)
    for r in (3, 1, 2):

        @pl.when(in_use(0))
        def _():
            cross(0, r).start()

        counted(r).start()

    for copy in load_small[1:]:
        copy.wait()
    held = [ref[...].astype(f32) for ref in held]
    for w in range(shares):
        for j in range(3):
            picked = jnp.zeros((1, held[j].shape[1]), f32)
            for source in range(shares):
                picked = jnp.where(writer[w] == source, held[j][source : source + 1], picked)
            s["snap_out"][w, j] = picked

    def regrouped(k):
        return send(
            s["snap_out"].at[flipped(group, k, shares)],
            snap_in.at[group],
            s["snap_send"].at[k],
            s["snap_got"].at[k],
            me,
            flipped(group, k, shares),
        )

    for k in range(1, shares):
        regrouped(k).start()
    snap_in[group] = s["snap_out"][group]

    def onward(t, c, w, way):
        place, there = orders[c].index(w), orders[c + way].index(w)
        return send(
            feats.at[t, 2 * place, pl.ds(1, 3)],
            feats.at[t, 2 * there, pl.ds(1, 3)],
            s["line_send"].at[t, (way + 1) // 2, place],
            s["feat_got"].at[t, 2 * there],
            me,
            group + 2 * way,
        )

    def moves(c, place):
        w = orders[c][place]
        ways = [way for way, goes in ((-1, w >= c), (1, w <= c)) if goes]
        return [(w, way) for way in ways if 0 <= c + way < len(orders)]

    def move_on(t, chips, place):
        for c in chips:

            @pl.when(chip == c)
            def _():
                for w, way in moves(c, place):

                    @pl.when(2 * w + core < used)
                    def _():
                        onward(t, c, w, way).start()

    def arrived(t, k):
        @pl.when(in_use(k))
        def _():
            to_twin(t, k - 1).wait_recv()

    def to_twin(t, k):
        return send(
            feats.at[t, k, pl.ds(1, 3)],
            feats.at[t, k + 1, pl.ds(1, 3)],
            s["twin_send"].at[t, k],
            s["feat_got"].at[t, k + 1],
            me,
            twin,
        )

    def start_total(m, carry):
        here = pl.ds(pl.multiple_of(m * tile, tile), tile)
        for t in range(2):
            total[t][here] = jnp.zeros((tile, units), f32)
        return carry

    lax.fori_loop(0, cols // tile, start_total, 0)
    load_own.wait()
    def far(t, axis, k):
        pair = (s["far_x"], s["got_x"]) if axis == 0 else (s["far_y"], s["got_y"])
        return send(
            pair[0].at[k, t],
            pair[1].at[k, t],
            s["far_send"].at[axis, t, k],
            s["far_got"].at[axis, t, k],
            square[1 + axis],
            group,
        )

    def last(axis, k):
        pair = (s["mid_y"], s["last_x"]) if axis == 0 else (s["mid_x"], s["last_y"])
        return send(
            pair[0].at[k],
            pair[1].at[k],
            s["last_send"].at[axis, k],
            s["last_got"].at[axis, k],
            square[1 + axis],
            group,
        )

    def spread(axis, k):
        return send(
            wide.at[k, :, 0],
            wide.at[k, :, 1 + axis],
            s["wide_send"].at[axis, k],
            s["wide_got"].at[axis, k],
            square[1 + axis],
            group,
        )

    def over(axis, k):
        here = low if axis == 0 else top
        return send(
            wide.at[k, :, 2 - axis, here],
            wide.at[k, :, 3, here],
            s["over_send"].at[axis, k],
            s["over_got"].at[axis, k],
            square[1 + axis],
            group,
        )

    def products(t, k):
        def column(i, carry):
            here = pl.ds(pl.multiple_of(i * tile, tile), tile)
            left = feats[t, k, pl.ds(1, 3)].reshape(3 * rows, cols)
            out = matmul(left, weights[t, :, here]).astype(bf16)
            part = [None] + [out[r * rows : (r + 1) * rows] for r in range(3)]
            s["far_x"][k, t, 0, :, here] = part[3][:half]
            s["far_x"][k, t, 1, :, here] = part[1][:half]
            s["far_y"][k, t, 0, :, here] = part[3][half:]
            s["far_y"][k, t, 1, :, here] = part[2][half:]
            s["mid_x"][k, t, :, here] = part[2][:half]
            s["mid_y"][k, t, :, here] = part[1][half:]
            return carry

        lax.fori_loop(0, units // tile, column, 0)
        far(t, 0, k).start()
        far(t, 1, k).start()


    def stage_products(k):
        at_end = (chip == outer[0]) | (chip == outer[1])
        within = jnp.logical_not(at_end)
        for t in (1, 0):

            @pl.when(k == 0)
            def _():
                load_weights[t].wait()

            @pl.when((k == 0) & in_use(0))
            def _():
                for r in (1, 2, 3):
                    cross(t, r).wait_recv()
                move_on(t, range(len(orders)), 0)

            @pl.when(k % 2 == 1)
            def _():
                arrived(t, k)

            @pl.when(k == 2)
            def _():
                arrived(t, 2)
                move_on(t, inner, 1)

            @pl.when((k == 2) & within)
            def _():
                arrived(t, 4)
                move_on(t, inner, 2)

            @pl.when((k == 4) & within)
            def _():
                arrived(t, 6)
                move_on(t, inner, 3)

            @pl.when((k >= 4) & (k % 2 == 0) & at_end)
            def _():
                arrived(t, k)

            @pl.when((k % 2 == 0) & in_use(k))
            def _():
                to_twin(t, k).start()

            @pl.when(in_use(k))
            def _():
                products(t, k)

            @pl.when((k == shares - 1) & jnp.logical_not(in_use(k)))
            def _():
                last_feats[t] = jnp.zeros(last_feats.shape[1:], bf16)
                wide[k, t] = jnp.zeros(wide.shape[2:], bf16)

    def own_rows(k):
        chosen = picker(k)

        def store_normed(r, here, values):
            feats[0, k, r, here] = values

        def store_masked(here, values):
            feats[1, k, 0, :, here] = values

        normal_rows(chosen, 1, store_normed)
        pick(chosen, s["own"], store_masked)

    def stage_own(k):
        @pl.when(k == 0)
        def _():
            for t in range(2):
                feats[t, 0, 0] = s["staged"][t, 0]

        @pl.when(k > 0)
        def _():
            own_rows(k)

        for t in range(2):

            def column(i, carry):
                here = pl.ds(pl.multiple_of(i * tile, tile), tile)
                out = matmul(feats[t, k, 0], weights[t, :, here])
                s["kept"][k, t, :, here] = out.astype(bf16)
                return carry

            lax.fori_loop(0, units // tile, column, 0)

            @pl.when(k == shares - 1)
            def _():
                for m in range(cols // tile):
                    here = pl.ds(m * tile, tile)
                    last_feats[t, here] = feats[t, k, :, :, here].reshape(4 * rows, tile).T

    def stage_middle(k):
        for t in range(2):
            far(t, 0, k).wait_recv()
            s["mid_x"][k, t] = rounded_sum(s["mid_x"][k, t], s["got_x"][k, t, 0])
        last(1, k).start()
        for t in range(2):
            far(t, 1, k).wait_recv()
            s["mid_y"][k, t] = rounded_sum(s["mid_y"][k, t], s["got_y"][k, t, 0])
        last(0, k).start()

    def stage_gelu(k):
        last(1, k).wait_recv()
        last(0, k).wait_recv()
        step = 16
        for axis, near_ref, last_ref in (
            (0, s["got_x"], s["last_y"]),
            (1, s["got_y"], s["last_x"]),
        ):

            def some(i, carry):
                here = pl.ds(pl.multiple_of(i * step, step), step)
                out = pl.ds(pl.multiple_of(axis * half + i * step, step), step)
                sums = [
                    s["kept"][k, t, out].astype(f32)
                    + near_ref[k, t, 1, here].astype(f32)
                    + last_ref[k, t, here].astype(f32)
                    for t in range(2)
                ]
                act, grad_pre = gelu_parts(*sums)
                wide[k, 0, 0, out] = grad_pre.astype(bf16)
                wide[k, 1, 0, out] = act.astype(bf16)
                return carry

            lax.fori_loop(0, half // step, some, 0)
        spread(0, k).start()
        spread(1, k).start()

    def stage_over(k):
        spread(0, k).wait_recv()
        over(1, k).start()
        spread(1, k).wait_recv()
        over(0, k).start()

    def stage_gradient(k):
        over(0, k).wait_recv()
        over(1, k).wait_recv()

        @pl.when(k < shares - 1)
        def _():
            for t in range(2):

                def some(m, carry):
                    here = pl.ds(pl.multiple_of(m * tile, tile), tile)
                    left = feats[t, k, :, :, here].reshape(4 * rows, tile)
                    right = wide[k, t].reshape(4 * rows, units)
                    total[t][here] = total[t][here] + outer_sum(left, right)
                    return carry

                lax.fori_loop(0, cols // tile, some, 0)

    def when_used(stage):
        def guarded(k):
            @pl.when(in_use(k))
            def _():
                stage(k)

        return guarded

    stages = [stage_middle, stage_gelu, stage_over, stage_gradient]
    stages = [stage_products] + [when_used(stage) for stage in stages]
    lags = list(enumerate(stages))
    lags = [lags[1], lags[0]] + lags[2:4] + [lags[4], (1, when_used(stage_own))]

    def pipeline(step, carry):
        for lag, stage in lags:

            @pl.when((step >= lag) & (step - lag < shares))
            def _():
                stage(step - lag)

        return carry

    lax.fori_loop(0, shares + len(stages) - 1, pipeline, 0)

    for k in range(1, shares):
        regrouped(k).wait()
    most[...] = s["counts"][0]
    for r in (1, 2, 3):
        counted(r).wait()
        most[...] = jnp.maximum(most[...], s["counts"][r])
    for t in range(2):

        @pl.when(in_use(0))
        def _():
            for r in (1, 2, 3):
                cross(t, r).wait_send()

        for k in range(0, shares, 2):

            @pl.when(in_use(k))
            def _():
                to_twin(t, k).wait_send()

    for c in range(len(orders)):

        @pl.when(chip == c)
        def _():
            for place in range(len(orders)):
                for w, way in moves(c, place):

                    @pl.when(2 * w + core < used)
                    def _():
                        for t in range(2):
                            onward(t, c, w, way).wait_send()

    def finish(k, carry):
        @pl.when(in_use(k))
        def _():
            for axis in range(2):
                for t in range(2):
                    far(t, axis, k).wait_send()
                last(axis, k).wait_send()
                spread(axis, k).wait_send()
                over(axis, k).wait_send()

        return carry

    lax.fori_loop(0, shares, finish, 0)


def last_kernel(
    total_up,
    total_down,
    feats,
    wide,
    snap,
    grad_up,
    grad_down,
    params,
    moments,
    ready,
    params_ready,
    moments_ready,
    sem,
    snap_sem,
):
    shares, rows, units = wide.shape[0], wide.shape[3], wide.shape[4]
    slots, tile = ready.shape[0], ready.shape[1]
    tiles = total_up.shape[0] // tile
    width = params.shape[1] // shares
    for source in range(shares):
        here = pl.ds(source * width, width)
        params_ready[:, here] = snap[source, 0].astype(params.dtype)
        for j in range(2):
            moments_ready[j, :, here] = snap[source, 1 + j]
    small = [
        pltpu.make_async_copy(params_ready, params, snap_sem.at[0]),
        pltpu.make_async_copy(moments_ready, moments, snap_sem.at[1]),
    ]
    for copy in small:
        copy.start()

    def written(n):
        t, m = n // tiles, n % tiles
        return pltpu.make_async_copy(
            ready.at[n % slots],
            (grad_up, grad_down)[t].at[pl.ds(m * tile, tile)],
            sem.at[n % slots],
        )

    for n in range(2 * tiles):
        t, here = n // tiles, pl.ds(n % tiles * tile, tile)
        if n >= slots:
            written(n - slots).wait()
        right = wide[shares - 1, t].reshape(4 * rows, units)
        ready[n % slots] = (total_up, total_down)[t][here] + matmul(feats[t, here], right)
        written(n).start()
    for n in range(max(0, 2 * tiles - slots), 2 * tiles):
        written(n).wait()
    for copy in small:
        copy.wait()


def weight_gradients(
    tokens,
    frame_mask,
    cotangent,
    up_weight,
    down_weight,
    snap_params,
    first_moment,
    second_moment,
    range_of_writer,
):
    shares = lax.axis_size("group")
    rows, (cols, units), flat = tokens.shape[0] // shares, up_weight.shape, snap_params.shape[1]
    types = [x.dtype for x in (snap_params, first_moment, second_moment)]
    buffers = scratch(shares, rows, cols, units, flat, types)
    anywhere = pl.BlockSpec(memory_space=pl.ANY)
    inside = pl.BlockSpec(memory_space=pltpu.VMEM)
    bf16, f32 = jnp.bfloat16, jnp.float32
    piece_flops = 8 * 4 * rows * cols * units

    def step(used):
        return pl.pallas_call(
            functools.partial(step_kernel, tuple(buffers), shares, used),
            out_shape=(
                pltpu.VMEM((cols, units), f32),
                pltpu.VMEM((cols, units), f32),
                pltpu.VMEM((2, cols, 4 * rows), bf16),
                pltpu.VMEM((shares, 2, 4, rows, units), bf16),
                pltpu.VMEM((shares, 3, 1, flat), f32),
                pltpu.VMEM((8, 128), f32),
            ),
            in_specs=[anywhere] * 9,
            out_specs=(inside,) * 6,
            scratch_shapes=list(buffers.values()),
            compiler_params=pltpu.CompilerParams(
                collective_id=shares - used, has_side_effects=True, vmem_limit_bytes=STEP_VMEM
            ),
            cost_estimate=pl.CostEstimate(
                flops=used * piece_flops,
                bytes_accessed=4 * cols * units + 4 * tokens.size,
                transcendentals=used * rows * units,
            ),
            name=f"backward_step_{used}",
        )(
            tokens,
            cotangent,
            up_weight,
            down_weight,
            frame_mask[None, :],
            snap_params,
            first_moment,
            second_moment,
            range_of_writer,
        )

    def finish(*sums):
        tile, slots = 256, 4
        return pl.pallas_call(
            last_kernel,
            out_shape=(
                jax.ShapeDtypeStruct((cols, units), f32),
                jax.ShapeDtypeStruct((cols, units), f32),
                jax.ShapeDtypeStruct((1, shares * flat), snap_params.dtype),
                jax.ShapeDtypeStruct((2, 1, shares * flat), first_moment.dtype),
            ),
            in_specs=[inside] * 5,
            out_specs=(anywhere,) * 4,
            scratch_shapes=[
                pltpu.VMEM((slots, tile, units), f32),
                pltpu.VMEM((1, shares * flat), snap_params.dtype),
                pltpu.VMEM((2, 1, shares * flat), first_moment.dtype),
                pltpu.SemaphoreType.DMA((slots,)),
                pltpu.SemaphoreType.DMA((2,)),
            ],
            compiler_params=pltpu.CompilerParams(vmem_limit_bytes=LAST_VMEM),
            cost_estimate=pl.CostEstimate(
                flops=piece_flops // 2, bytes_accessed=8 * cols * units, transcendentals=0
            ),
            name="last_piece",
        )(*sums)

    fewer = shares - 1
    *sums, most = step(fewer)
    results = finish(*sums)
    return lax.cond(
        most[0, 0] > fewer * rows, lambda done: finish(*step(shares)[:5]), lambda done: done, results
    )


def weight_gradients_any(tokens, frame_mask, cotangent, up_weight, down_weight, *snapshot):
    shares = lax.axis_size("group")
    group = lax.axis_index("group")
    mask = own_part(frame_mask, shares, group)[:, None].astype(jnp.bfloat16)

    def to_features(rows_here):
        part = lax.all_to_all(rows_here, "dp", split_axis=1, concat_axis=0, tiled=True)
        return lax.all_gather(part, "group", axis=0, tiled=True)

    def own_rows_total(left, weight):
        part = matmul(left, weight).astype(jnp.bfloat16)
        return lax.psum_scatter(part, "dp", scatter_dimension=0, tiled=True).astype(jnp.float32)

    normed = to_features(normalize(own_part(tokens, shares, group)))
    masked = to_features(own_part(cotangent, shares, group) * mask)
    act, grad_pre = gelu_pair(
        own_rows_total(normed, up_weight), own_rows_total(masked, down_weight)
    )
    grad_down = outer_sum(masked, lax.all_gather(act, "dp", axis=0, tiled=True))
    grad_up = outer_sum(normed, lax.all_gather(grad_pre, "dp", axis=0, tiled=True))
    return grad_up, grad_down, *regroup(*snapshot)


def per_device(
    tokens,
    frame_mask,
    cotangent,
    up_weight,
    down_weight,
    snap_params,
    first_moment,
    second_moment,
    range_of_writer,
):
    square = fits_square(tokens, up_weight)
    compute = weight_gradients if square else weight_gradients_any
    snapshot = (snap_params, first_moment, second_moment, range_of_writer)
    return compute(tokens, frame_mask, cotangent, up_weight, down_weight, *snapshot)


def solution(mesh):
    placed = (
        P("dp", None),
        P("dp"),
        P("dp", None),
        P("dp", "group"),
        P("dp", "group"),
        P(None, ("dp", "group")),
        P(None, ("dp", "group")),
        P(None, ("dp", "group")),
        P(),
    )
    return jax.shard_map(
        per_device,
        mesh=mesh,
        in_specs=placed,
        out_specs=(P("dp", "group"), P("dp", "group"), P("group", "dp"), P(None, "group", "dp")),
        check_vma=False,
    )
```

```python
import functools

import jax
import jax.numpy as jnp
from jax import lax
from jax.experimental import pallas as pl
from jax.experimental.pallas import tpu as pltpu
from jax.sharding import PartitionSpec as P

EPS = 1e-06
STEP_VMEM, LAST_VMEM = 41 * 2**20, 8 * 2**20


def normalize(tokens):
    values = tokens.astype(jnp.float32)
    centred = values - jnp.mean(values, axis=1, keepdims=True)
    spread = jnp.mean(centred * centred, axis=1, keepdims=True)
    return (centred * lax.rsqrt(spread + EPS)).astype(jnp.bfloat16)


def gelu_pair(pre, d_act):
    act, pullback = jax.vjp(lambda v: jax.nn.gelu(v, approximate=True), pre)
    return (act.astype(jnp.bfloat16), pullback(d_act)[0].astype(jnp.bfloat16))


def outer_sum(left, right):
    return lax.dot_general(
        left, right, (((0,), (0,)), ((), ())), preferred_element_type=jnp.float32
    )


def regroup(snap_params, first_moment, second_moment, range_of_writer):
    flat = snap_params.shape[1]
    held = jnp.concatenate(
        [snap_params, first_moment.astype(jnp.bfloat16), second_moment.astype(jnp.bfloat16)],
        axis=1,
    )
    send = jnp.take(held, range_of_writer, axis=0).reshape(-1, 3, flat)
    got = lax.all_to_all(send, "group", split_axis=0, concat_axis=0, tiled=True)
    lines = jnp.swapaxes(got, 0, 1).reshape(3, 1, -1)
    return lines[0], lines[1:].astype(first_moment.dtype)


def matmul(left, right):
    return jnp.dot(left, right, preferred_element_type=jnp.float32)


def own_part(values, parts, part):
    rows = values.shape[0] // parts
    return lax.dynamic_slice_in_dim(values, part * rows, rows, axis=0)


def rounded_sum(left, right):
    total = left.astype(jnp.float32) + right.astype(jnp.float32)
    return total.astype(jnp.bfloat16)


def fits_square(tokens, up_weight):
    shares = lax.axis_size("group")
    rows, features = tokens.shape
    return (
        lax.axis_size("dp") == 4
        and shares == 8
        and rows % (32 * shares) == 0
        and up_weight.shape[0] * 4 == features
        and up_weight.shape[0] % 256 == 0
        and up_weight.shape[1] % 256 == 0
    )


def flipped(index, mask, size):
    out, bit = index, 1
    while bit < size:
        out = out + bit * ((mask // bit) % 2) * (1 - 2 * ((index // bit) % 2))
        bit *= 2
    return out


def line_orders(chips):
    return [sorted(range(chips), key=lambda w: (abs(w - c), w)) for c in range(chips)]


def gelu_parts(pre, d_act):
    scale, cubic = 0.7978845608028654, 0.044715
    square = pre * pre
    wave = jnp.tanh(scale * (pre + cubic * (square * pre)))
    half = 0.5 * (1.0 + wave)
    slope = half + 0.5 * pre * (1.0 - wave * wave) * (scale * (1.0 + 3.0 * cubic * square))
    return pre * half, d_act * slope


def scratch(shares, rows, cols, units, flat, types):
    half, bf16, f32 = rows // 2, jnp.bfloat16, jnp.float32
    dma = pltpu.SemaphoreType.DMA
    return {
        "feats": pltpu.VMEM((2, shares, 4, rows, cols), bf16),
        "weights": pltpu.VMEM((2, cols, units), bf16),
        "lines": pltpu.VMEM((4, shares * rows, cols), bf16),
        "packed": pltpu.VMEM((4, rows, cols), bf16),
        "slot": pltpu.VMEM((1, shares * rows), jnp.int32),
        "counts": pltpu.VMEM((4, 8, 128), f32),
        "own": pltpu.VMEM((shares * rows, cols), bf16),
        "staged": pltpu.VMEM((2, 4, rows, cols), bf16),
        "far_x": pltpu.VMEM((shares, 2, 2, half, units), bf16),
        "far_y": pltpu.VMEM((shares, 2, 2, half, units), bf16),
        "kept": pltpu.VMEM((shares, 2, rows, units), bf16),
        "mid_x": pltpu.VMEM((shares, 2, half, units), bf16),
        "mid_y": pltpu.VMEM((shares, 2, half, units), bf16),
        "got_x": pltpu.VMEM((shares, 2, 2, half, units), bf16),
        "got_y": pltpu.VMEM((shares, 2, 2, half, units), bf16),
        "last_x": pltpu.VMEM((shares, 2, half, units), bf16),
        "last_y": pltpu.VMEM((shares, 2, half, units), bf16),
        "snap_out": pltpu.VMEM((shares, 3, 1, flat), f32),
        "mask": pltpu.VMEM((1, shares * rows), jnp.int32),
        "held_params": pltpu.VMEM((shares, flat), types[0]),
        "held_first": pltpu.VMEM((shares, flat), types[1]),
        "held_second": pltpu.VMEM((shares, flat), types[2]),
        "writer": pltpu.SMEM((shares,), jnp.int32),
        "small_sem": dma((5,)),
        "line_sem": dma((4,)),
        "own_sem": dma((1,)),
        "count_send": dma((4,)),
        "count_got": dma((4,)),
        "weight_sem": dma((2,)),
        "cross_send": dma((2, 4)),
        "cross_got": dma((2, 4)),
        "line_send": dma((2, 2, shares // 2)),
        "twin_send": dma((2, shares)),
        "feat_got": dma((2, shares)),
        "far_send": dma((2, 2, shares)),
        "far_got": dma((2, 2, shares)),
        "last_send": dma((2, shares)),
        "last_got": dma((2, shares)),
        "wide_send": dma((2, shares)),
        "wide_got": dma((2, shares)),
        "over_send": dma((2, shares)),
        "over_got": dma((2, shares)),
        "snap_send": dma((shares,)),
        "snap_got": dma((shares,)),
    }


def step_kernel(names, shares, used, *refs):
    tokens, cotangent, up_weight, down_weight, *small = refs[:9]
    *total, last_feats, wide, snap_in, most = refs[9:15]
    s = dict(zip(names, refs[15:]))
    feats, weights, mask, writer = s["feats"], s["weights"], s["mask"], s["writer"]
    held = [s["held_params"], s["held_first"], s["held_second"]]
    me, group = lax.axis_index("dp"), lax.axis_index("group")
    square = [me, me + 1 - 2 * (me % 2), me + 2 - 4 * (me // 2), 3 - me]
    twin = flipped(group, 1, shares)
    chip, core = group // 2, group % 2
    orders = line_orders(shares // 2)
    inner = range(1, len(orders) - 1)
    outer = (0, len(orders) - 1)
    table = sum(w << (8 * c + 2 * p) for c, order in enumerate(orders) for p, w in enumerate(order))
    own_order = table // ((1 + 255 * (chip % 2)) * (1 + 65535 * (chip // 2))) % 256
    rows, cols, units = feats.shape[3], feats.shape[4], weights.shape[2]
    half, tile = rows // 2, 256
    bf16, f32 = jnp.bfloat16, jnp.float32
    top, low = pl.ds(0, half), pl.ds(half, half)

    def send(src, dst, send_sem, got_sem, dp_to, group_to):
        return pltpu.make_async_remote_copy(
            src_ref=src,
            dst_ref=dst,
            send_sem=send_sem,
            recv_sem=got_sem,
            device_id=(dp_to, group_to),
            device_id_type=pl.DeviceIdType.MESH,
        )

    barrier = pltpu.get_barrier_semaphore()
    partners = [(d, group) for d in square[1:]]
    partners += [(me, flipped(group, k, shares)) for k in range(1, shares)]
    for there in partners:
        pl.semaphore_signal(
            barrier, inc=1, device_id=there, device_id_type=pl.DeviceIdType.MESH
        )

    def owner_of(k):
        place = k // 2
        there = own_order // ((1 + 3 * (place % 2)) * (1 + 15 * (place // 2))) % 4
        return 2 * there + (core + k) % 2

    def in_use(k):
        return owner_of(k) < used

    def columns_of(r):
        return pl.ds(pl.multiple_of(square[r] * cols, cols), cols)

    def load_lines(source, r):
        return pltpu.make_async_copy(
            source.at[:, columns_of(r)], s["lines"].at[r], s["line_sem"].at[r]
        )

    load_own = pltpu.make_async_copy(
        cotangent.at[:, columns_of(0)], s["own"], s["own_sem"].at[0]
    )
    load_weights = [
        pltpu.make_async_copy(w, weights.at[t], s["weight_sem"].at[t])
        for t, w in enumerate((up_weight, down_weight))
    ]
    load_small = [
        pltpu.make_async_copy(src, dst, s["small_sem"].at[n])
        for n, (src, dst) in enumerate(zip(small, [mask] + held + [writer]))
    ]
    load_small[0].start()
    for r in (1, 2, 3, 0):
        load_lines(cotangent, r).start()
    for copy in load_small[1:]:
        copy.start()

    def rows_to_slots():
        load_small[0].wait()
        count = mask.shape[1]
        row = lax.broadcasted_iota(jnp.int32, (count, count), 0)
        column = lax.broadcasted_iota(jnp.int32, (count, count), 1)
        before = jnp.where(row < column, 1.0, 0.0).astype(bf16)
        ones = jnp.broadcast_to(mask[...].astype(f32), (8, count))
        places = matmul(ones.astype(bf16), before)[:1].astype(jnp.int32)
        s["slot"][...] = jnp.where(mask[...] > 0, places, -1)
        held_here = jnp.sum(ones, axis=1, keepdims=True)
        s["counts"][0] = jnp.broadcast_to(held_here, (8, 128))

    def picker(k):
        shape = (rows, mask.shape[1])
        at = lax.broadcasted_iota(jnp.int32, shape, 0) + owner_of(k) * rows
        return jnp.where(at == s["slot"][...], 1.0, 0.0).astype(bf16)

    def pick(chosen, source, store):
        store(pl.ds(0, cols), matmul(chosen, source[...]).astype(bf16))

    def normal_rows(chosen, parts, store):
        for r in range(4):

            def keep(here, values):
                s["packed"][r, :, here] = values

            pick(chosen, s["lines"].at[r], keep)
        step = 16

        def some(i, carry):
            here = pl.ds(pl.multiple_of(i * step, step), step)
            values = [s["packed"][r, here].astype(f32) for r in range(4)]
            mean = sum(jnp.sum(v, axis=1, keepdims=True) for v in values) / (4 * cols)
            centred = [v - mean for v in values]
            squares = sum(jnp.sum(c * c, axis=1, keepdims=True) for c in centred)
            scale = lax.rsqrt(squares / (4 * cols) + EPS)
            for r in range(parts):
                store(r, here, (centred[r] * scale).astype(bf16))
            return carry

        lax.fori_loop(0, rows // step, some, 0)

    def cross(t, r):
        return send(
            s["staged"].at[t, r],
            feats.at[t, 0, r],
            s["cross_send"].at[t, r],
            s["cross_got"].at[t, r],
            square[r],
            group,
        )

    def counted(r):
        return send(
            s["counts"].at[0],
            s["counts"].at[r],
            s["count_send"].at[r],
            s["count_got"].at[r],
            square[r],
            group,
        )

    def store_staged(r, here, values):
        s["staged"][0, r, here] = values

    rows_to_slots()
    chosen = picker(0)
    for n, r in enumerate((1, 2, 3, 0)):
        load_lines(cotangent, r).wait()

        def keep(here, values):
            s["staged"][1, r, :, here] = values

        pick(chosen, s["lines"].at[r], keep)
        load_lines(tokens, r).start()
        if n == 0:
            pl.semaphore_wait(barrier, len(partners))
        if r:

            @pl.when(in_use(0))
            def _():
                cross(1, r).start()

    for copy in load_weights:
        copy.start()
    load_own.start()
    for r in range(4):
        load_lines(tokens, r).wait()
    normal_rows(chosen, 4, store_staged)
    for r in (3, 1, 2):

        @pl.when(in_use(0))
        def _():
            cross(0, r).start()

        counted(r).start()

    for copy in load_small[1:]:
        copy.wait()
    held = [ref[...].astype(f32) for ref in held]
    for w in range(shares):
        for j in range(3):
            picked = jnp.zeros((1, held[j].shape[1]), f32)
            for source in range(shares):
                picked = jnp.where(writer[w] == source, held[j][source : source + 1], picked)
            s["snap_out"][w, j] = picked

    def regrouped(k):
        return send(
            s["snap_out"].at[flipped(group, k, shares)],
            snap_in.at[group],
            s["snap_send"].at[k],
            s["snap_got"].at[k],
            me,
            flipped(group, k, shares),
        )

    for k in range(1, shares):
        regrouped(k).start()
    snap_in[group] = s["snap_out"][group]

    def onward(t, c, w, way):
        place, there = orders[c].index(w), orders[c + way].index(w)
        return send(
            feats.at[t, 2 * place, pl.ds(1, 3)],
            feats.at[t, 2 * there, pl.ds(1, 3)],
            s["line_send"].at[t, (way + 1) // 2, place],
            s["feat_got"].at[t, 2 * there],
            me,
            group + 2 * way,
        )

    def moves(c, place):
        w = orders[c][place]
        ways = [way for way, goes in ((-1, w >= c), (1, w <= c)) if goes]
        return [(w, way) for way in ways if 0 <= c + way < len(orders)]

    def move_on(t, chips, place):
        for c in chips:

            @pl.when(chip == c)
            def _():
                for w, way in moves(c, place):

                    @pl.when(2 * w + core < used)
                    def _():
                        onward(t, c, w, way).start()

    def arrived(t, k):
        @pl.when(in_use(k))
        def _():
            to_twin(t, k - 1).wait_recv()

    def to_twin(t, k):
        return send(
            feats.at[t, k, pl.ds(1, 3)],
            feats.at[t, k + 1, pl.ds(1, 3)],
            s["twin_send"].at[t, k],
            s["feat_got"].at[t, k + 1],
            me,
            twin,
        )

    def start_total(m, carry):
        here = pl.ds(pl.multiple_of(m * tile, tile), tile)
        for t in range(2):
            total[t][here] = jnp.zeros((tile, units), f32)
        return carry

    lax.fori_loop(0, cols // tile, start_total, 0)
    load_own.wait()
    def far(t, axis, k):
        pair = (s["far_x"], s["got_x"]) if axis == 0 else (s["far_y"], s["got_y"])
        return send(
            pair[0].at[k, t],
            pair[1].at[k, t],
            s["far_send"].at[axis, t, k],
            s["far_got"].at[axis, t, k],
            square[1 + axis],
            group,
        )

    def last(axis, k):
        pair = (s["mid_y"], s["last_x"]) if axis == 0 else (s["mid_x"], s["last_y"])
        return send(
            pair[0].at[k],
            pair[1].at[k],
            s["last_send"].at[axis, k],
            s["last_got"].at[axis, k],
            square[1 + axis],
            group,
        )

    def spread(axis, k):
        return send(
            wide.at[k, :, 0],
            wide.at[k, :, 1 + axis],
            s["wide_send"].at[axis, k],
            s["wide_got"].at[axis, k],
            square[1 + axis],
            group,
        )

    def over(axis, k):
        here = low if axis == 0 else top
        return send(
            wide.at[k, :, 2 - axis, here],
            wide.at[k, :, 3, here],
            s["over_send"].at[axis, k],
            s["over_got"].at[axis, k],
            square[1 + axis],
            group,
        )

    def products(t, k):
        def column(i, carry):
            here = pl.ds(pl.multiple_of(i * tile, tile), tile)
            left = feats[t, k, pl.ds(1, 3)].reshape(3 * rows, cols)
            out = matmul(left, weights[t, :, here]).astype(bf16)
            part = [None] + [out[r * rows : (r + 1) * rows] for r in range(3)]
            s["far_x"][k, t, 0, :, here] = part[3][:half]
            s["far_x"][k, t, 1, :, here] = part[1][:half]
            s["far_y"][k, t, 0, :, here] = part[3][half:]
            s["far_y"][k, t, 1, :, here] = part[2][half:]
            s["mid_x"][k, t, :, here] = part[2][:half]
            s["mid_y"][k, t, :, here] = part[1][half:]
            return carry

        lax.fori_loop(0, units // tile, column, 0)
        far(t, 0, k).start()
        far(t, 1, k).start()


    def stage_products(k):
        at_end = (chip == outer[0]) | (chip == outer[1])
        within = jnp.logical_not(at_end)
        for t in (1, 0):

            @pl.when(k == 0)
            def _():
                load_weights[t].wait()

            @pl.when((k == 0) & in_use(0))
            def _():
                for r in (1, 2, 3):
                    cross(t, r).wait_recv()
                move_on(t, range(len(orders)), 0)

            @pl.when(k % 2 == 1)
            def _():
                arrived(t, k)

            @pl.when(k == 2)
            def _():
                arrived(t, 2)
                move_on(t, inner, 1)

            @pl.when((k == 2) & within)
            def _():
                arrived(t, 4)
                move_on(t, inner, 2)

            @pl.when((k == 4) & within)
            def _():
                arrived(t, 6)
                move_on(t, inner, 3)

            @pl.when((k >= 4) & (k % 2 == 0) & at_end)
            def _():
                arrived(t, k)

            @pl.when((k % 2 == 0) & in_use(k))
            def _():
                to_twin(t, k).start()

            @pl.when(in_use(k))
            def _():
                products(t, k)

            @pl.when((k == shares - 1) & jnp.logical_not(in_use(k)))
            def _():
                last_feats[t] = jnp.zeros(last_feats.shape[1:], bf16)
                wide[k, t] = jnp.zeros(wide.shape[2:], bf16)

    def own_rows(k):
        chosen = picker(k)

        def store_normed(r, here, values):
            feats[0, k, r, here] = values

        def store_masked(here, values):
            feats[1, k, 0, :, here] = values

        normal_rows(chosen, 1, store_normed)
        pick(chosen, s["own"], store_masked)

    def stage_own(k):
        @pl.when(k == 0)
        def _():
            for t in range(2):
                feats[t, 0, 0] = s["staged"][t, 0]

        @pl.when(k > 0)
        def _():
            own_rows(k)

        for t in range(2):

            def column(i, carry):
                here = pl.ds(pl.multiple_of(i * tile, tile), tile)
                out = matmul(feats[t, k, 0], weights[t, :, here])
                s["kept"][k, t, :, here] = out.astype(bf16)
                return carry

            lax.fori_loop(0, units // tile, column, 0)

            @pl.when(k == shares - 1)
            def _():
                for m in range(cols // tile):
                    here = pl.ds(m * tile, tile)
                    last_feats[t, here] = feats[t, k, :, :, here].reshape(4 * rows, tile).T

    def stage_middle(k):
        for t in range(2):
            far(t, 0, k).wait_recv()
            s["mid_x"][k, t] = rounded_sum(s["mid_x"][k, t], s["got_x"][k, t, 0])
        last(1, k).start()
        for t in range(2):
            far(t, 1, k).wait_recv()
            s["mid_y"][k, t] = rounded_sum(s["mid_y"][k, t], s["got_y"][k, t, 0])
        last(0, k).start()

    def stage_gelu(k):
        last(1, k).wait_recv()
        last(0, k).wait_recv()
        step = 16
        for axis, near_ref, last_ref in (
            (0, s["got_x"], s["last_y"]),
            (1, s["got_y"], s["last_x"]),
        ):

            def some(i, carry):
                here = pl.ds(pl.multiple_of(i * step, step), step)
                out = pl.ds(pl.multiple_of(axis * half + i * step, step), step)
                sums = [
                    s["kept"][k, t, out].astype(f32)
                    + near_ref[k, t, 1, here].astype(f32)
                    + last_ref[k, t, here].astype(f32)
                    for t in range(2)
                ]
                act, grad_pre = gelu_parts(*sums)
                wide[k, 0, 0, out] = grad_pre.astype(bf16)
                wide[k, 1, 0, out] = act.astype(bf16)
                return carry

            lax.fori_loop(0, half // step, some, 0)
        spread(0, k).start()
        spread(1, k).start()

    def stage_over(k):
        spread(0, k).wait_recv()
        over(1, k).start()
        spread(1, k).wait_recv()
        over(0, k).start()

    def stage_gradient(k):
        over(0, k).wait_recv()
        over(1, k).wait_recv()

        @pl.when(k < shares - 1)
        def _():
            for t in range(2):

                def some(m, carry):
                    here = pl.ds(pl.multiple_of(m * tile, tile), tile)
                    left = feats[t, k, :, :, here].reshape(4 * rows, tile)
                    right = wide[k, t].reshape(4 * rows, units)
                    total[t][here] = total[t][here] + outer_sum(left, right)
                    return carry

                lax.fori_loop(0, cols // tile, some, 0)

    def when_used(stage):
        def guarded(k):
            @pl.when(in_use(k))
            def _():
                stage(k)

        return guarded

    stages = [stage_middle, stage_gelu, stage_over, stage_gradient]
    stages = [stage_products] + [when_used(stage) for stage in stages]
    lags = list(enumerate(stages))
    lags = [lags[1], lags[0]] + lags[2:4] + [lags[4], (1, when_used(stage_own))]

    def pipeline(step, carry):
        for lag, stage in lags:

            @pl.when((step >= lag) & (step - lag < shares))
            def _():
                stage(step - lag)

        return carry

    lax.fori_loop(0, shares + len(stages) - 1, pipeline, 0)

    for k in range(1, shares):
        regrouped(k).wait()
    most[...] = s["counts"][0]
    for r in (1, 2, 3):
        counted(r).wait()
        most[...] = jnp.maximum(most[...], s["counts"][r])
    for t in range(2):

        @pl.when(in_use(0))
        def _():
            for r in (1, 2, 3):
                cross(t, r).wait_send()

        for k in range(0, shares, 2):

            @pl.when(in_use(k))
            def _():
                to_twin(t, k).wait_send()

    for c in range(len(orders)):

        @pl.when(chip == c)
        def _():
            for place in range(len(orders)):
                for w, way in moves(c, place):

                    @pl.when(2 * w + core < used)
                    def _():
                        for t in range(2):
                            onward(t, c, w, way).wait_send()

    def finish(k, carry):
        @pl.when(in_use(k))
        def _():
            for axis in range(2):
                for t in range(2):
                    far(t, axis, k).wait_send()
                last(axis, k).wait_send()
                spread(axis, k).wait_send()
                over(axis, k).wait_send()

        return carry

    lax.fori_loop(0, shares, finish, 0)


def last_kernel(
    total_up,
    total_down,
    feats,
    wide,
    snap,
    grad_up,
    grad_down,
    params,
    moments,
    ready,
    params_ready,
    moments_ready,
    sem,
    snap_sem,
):
    shares, rows, units = wide.shape[0], wide.shape[3], wide.shape[4]
    slots, tile = ready.shape[0], ready.shape[1]
    tiles = total_up.shape[0] // tile
    width = params.shape[1] // shares
    for source in range(shares):
        here = pl.ds(source * width, width)
        params_ready[:, here] = snap[source, 0].astype(params.dtype)
        for j in range(2):
            moments_ready[j, :, here] = snap[source, 1 + j]
    small = [
        pltpu.make_async_copy(params_ready, params, snap_sem.at[0]),
        pltpu.make_async_copy(moments_ready, moments, snap_sem.at[1]),
    ]
    for copy in small:
        copy.start()

    def written(n):
        t, m = n // tiles, n % tiles
        return pltpu.make_async_copy(
            ready.at[n % slots],
            (grad_up, grad_down)[t].at[pl.ds(m * tile, tile)],
            sem.at[n % slots],
        )

    for n in range(2 * tiles):
        t, here = n // tiles, pl.ds(n % tiles * tile, tile)
        if n >= slots:
            written(n - slots).wait()
        right = wide[shares - 1, t].reshape(4 * rows, units)
        ready[n % slots] = (total_up, total_down)[t][here] + matmul(feats[t, here], right)
        written(n).start()
    for n in range(max(0, 2 * tiles - slots), 2 * tiles):
        written(n).wait()
    for copy in small:
        copy.wait()


def weight_gradients(
    tokens,
    frame_mask,
    cotangent,
    up_weight,
    down_weight,
    snap_params,
    first_moment,
    second_moment,
    range_of_writer,
):
    shares = lax.axis_size("group")
    rows, (cols, units), flat = tokens.shape[0] // shares, up_weight.shape, snap_params.shape[1]
    types = [x.dtype for x in (snap_params, first_moment, second_moment)]
    buffers = scratch(shares, rows, cols, units, flat, types)
    anywhere = pl.BlockSpec(memory_space=pl.ANY)
    inside = pl.BlockSpec(memory_space=pltpu.VMEM)
    bf16, f32 = jnp.bfloat16, jnp.float32
    piece_flops = 8 * 4 * rows * cols * units

    def step(used):
        return pl.pallas_call(
            functools.partial(step_kernel, tuple(buffers), shares, used),
            out_shape=(
                pltpu.VMEM((cols, units), f32),
                pltpu.VMEM((cols, units), f32),
                pltpu.VMEM((2, cols, 4 * rows), bf16),
                pltpu.VMEM((shares, 2, 4, rows, units), bf16),
                pltpu.VMEM((shares, 3, 1, flat), f32),
                pltpu.VMEM((8, 128), f32),
            ),
            in_specs=[anywhere] * 9,
            out_specs=(inside,) * 6,
            scratch_shapes=list(buffers.values()),
            compiler_params=pltpu.CompilerParams(
                collective_id=shares - used, has_side_effects=True, vmem_limit_bytes=STEP_VMEM
            ),
            cost_estimate=pl.CostEstimate(
                flops=used * piece_flops,
                bytes_accessed=4 * cols * units + 4 * tokens.size,
                transcendentals=used * rows * units,
            ),
            name=f"backward_step_{used}",
        )(
            tokens,
            cotangent,
            up_weight,
            down_weight,
            frame_mask[None, :],
            snap_params,
            first_moment,
            second_moment,
            range_of_writer,
        )

    def finish(*sums):
        tile, slots = 256, 5
        return pl.pallas_call(
            last_kernel,
            out_shape=(
                jax.ShapeDtypeStruct((cols, units), f32),
                jax.ShapeDtypeStruct((cols, units), f32),
                jax.ShapeDtypeStruct((1, shares * flat), snap_params.dtype),
                jax.ShapeDtypeStruct((2, 1, shares * flat), first_moment.dtype),
            ),
            in_specs=[inside] * 5,
            out_specs=(anywhere,) * 4,
            scratch_shapes=[
                pltpu.VMEM((slots, tile, units), f32),
                pltpu.VMEM((1, shares * flat), snap_params.dtype),
                pltpu.VMEM((2, 1, shares * flat), first_moment.dtype),
                pltpu.SemaphoreType.DMA((slots,)),
                pltpu.SemaphoreType.DMA((2,)),
            ],
            compiler_params=pltpu.CompilerParams(vmem_limit_bytes=LAST_VMEM),
            cost_estimate=pl.CostEstimate(
                flops=piece_flops // 2, bytes_accessed=8 * cols * units, transcendentals=0
            ),
            name="last_piece",
        )(*sums)

    fewer = shares - 1
    *sums, most = step(fewer)
    results = finish(*sums)
    return lax.cond(
        most[0, 0] > fewer * rows, lambda done: finish(*step(shares)[:5]), lambda done: done, results
    )


def weight_gradients_any(tokens, frame_mask, cotangent, up_weight, down_weight, *snapshot):
    shares = lax.axis_size("group")
    group = lax.axis_index("group")
    mask = own_part(frame_mask, shares, group)[:, None].astype(jnp.bfloat16)

    def to_features(rows_here):
        part = lax.all_to_all(rows_here, "dp", split_axis=1, concat_axis=0, tiled=True)
        return lax.all_gather(part, "group", axis=0, tiled=True)

    def own_rows_total(left, weight):
        part = matmul(left, weight).astype(jnp.bfloat16)
        return lax.psum_scatter(part, "dp", scatter_dimension=0, tiled=True).astype(jnp.float32)

    normed = to_features(normalize(own_part(tokens, shares, group)))
    masked = to_features(own_part(cotangent, shares, group) * mask)
    act, grad_pre = gelu_pair(
        own_rows_total(normed, up_weight), own_rows_total(masked, down_weight)
    )
    grad_down = outer_sum(masked, lax.all_gather(act, "dp", axis=0, tiled=True))
    grad_up = outer_sum(normed, lax.all_gather(grad_pre, "dp", axis=0, tiled=True))
    return grad_up, grad_down, *regroup(*snapshot)


def per_device(
    tokens,
    frame_mask,
    cotangent,
    up_weight,
    down_weight,
    snap_params,
    first_moment,
    second_moment,
    range_of_writer,
):
    square = fits_square(tokens, up_weight)
    compute = weight_gradients if square else weight_gradients_any
    snapshot = (snap_params, first_moment, second_moment, range_of_writer)
    return compute(tokens, frame_mask, cotangent, up_weight, down_weight, *snapshot)


def solution(mesh):
    placed = (
        P("dp", None),
        P("dp"),
        P("dp", None),
        P("dp", "group"),
        P("dp", "group"),
        P(None, ("dp", "group")),
        P(None, ("dp", "group")),
        P(None, ("dp", "group")),
        P(),
    )
    return jax.shard_map(
        per_device,
        mesh=mesh,
        in_specs=placed,
        out_specs=(P("dp", "group"), P("dp", "group"), P("group", "dp"), P(None, "group", "dp")),
        check_vma=False,
    )
```
